32 devices in a mesh: dp: 4 (over y, z), tp: 8 (over x, core).
Axes of the slice: x: 4, y: 2, z: 2, core: 2. Of those that a mesh axis runs over, the one named last changes fastest.
The devices are a block of a 4x4x8 slice.
Arguments:
- x: bfloat16 [768, 2048], P('dp'), parts along dimension 0
- lengths: int32 [260], P('dp'), parts along dimension 0
- attn_gain: bfloat16 [2, 2048], replicated
- w_q: bfloat16 [2, 2048, 2048], P(None, None, 'tp')
- w_k: bfloat16 [2, 2048, 512], P(None, None, 'tp')
- w_v: bfloat16 [2, 2048, 512], P(None, None, 'tp')
- w_o: bfloat16 [2, 2048, 2048], P(None, 'tp')
- mlp_gain: bfloat16 [2, 2048], replicated
- w_gate: bfloat16 [2, 2048, 8192], P(None, None, 'tp')
- w_up: bfloat16 [2, 2048, 8192], P(None, None, 'tp')
- w_down: bfloat16 [2, 8192, 2048], P(None, 'tp')
- k_cache: bfloat16 [2, 260, 8, 1024, 64], P(None, 'dp', 'tp'), parts along dimension 1
- v_cache: bfloat16 [2, 260, 8, 1024, 64], P(None, 'dp', 'tp'), parts along dimension 1
Outputs:
- output: bfloat16 [768, 2048], P('dp'), parts along dimension 0
There are 4 independent parts. The reference program is written for one: setup_inputs(seed, part) draws one part's arguments, and reference() takes and returns one part's arrays. A program takes and returns all parts, laid end to end along the dimension named above; an argument that names none is the same for every part.
All inputs are finite; a program needn't handle non-finite values.
Results may differ from the reference program's by a relative error of at most 0.02.
Values are sent between devices in bfloat16 or wider.
A program may use at most 768 MiB of HBM per device.

```python
import jax
import jax.numpy as jnp
from jax import lax

D = 2048
HEADS = 32
KV_HEADS = 8
HEAD = 64
FF = 8192
BATCH = 64
CHUNK = 128
SEQ = 1024
LAYERS = 2

GROUP = HEADS // KV_HEADS
TOKENS = BATCH + CHUNK
ATTN_SCALE = HEAD ** -0.5
ROPE_BASE = 500000.0
EPSILON = 1e-5


def setup_inputs(seed: int = 0, part: int = 0) -> dict:
    root_key = jax.random.key(seed)
    shared_keys = jax.random.split(root_key, 9)
    part_keys = jax.random.split(jax.random.fold_in(root_key, part), 8)

    def gaussian(sub_key, arr_shape, factor):
        return jax.random.normal(sub_key, arr_shape, jnp.float32) * factor

    lengths = jax.random.randint(part_keys[1], (BATCH + 1,), 1, SEQ)
    longest = jax.random.randint(part_keys[2], (), 0, BATCH + 1)
    lengths = jnp.where(jnp.arange(BATCH + 1) == longest, SEQ - 1, lengths).astype(jnp.int32)
    pos_ramp = (jnp.arange(SEQ, dtype=jnp.float32) * (2.0 / SEQ) - 1.0)[:, None]
    cache_shape = (LAYERS, BATCH + 1, KV_HEADS, SEQ, HEAD)
    row_shape = (LAYERS, BATCH + 1, KV_HEADS, 1, HEAD)
    k_cache = gaussian(part_keys[3], cache_shape, 1.0) + pos_ramp * gaussian(part_keys[4], row_shape, 1.0)
    v_cache = gaussian(part_keys[5], row_shape, 1.0) + pos_ramp * gaussian(part_keys[6], row_shape, 1.0) + gaussian(part_keys[7], cache_shape, 0.5)
    return {
        'x': gaussian(part_keys[0], (TOKENS, D), 1.0).astype(jnp.bfloat16),
        'lengths': lengths,
        'attn_gain': jax.random.uniform(shared_keys[0], (LAYERS, D), jnp.float32, 0.5, 1.5).astype(jnp.bfloat16),
        'w_q': gaussian(shared_keys[1], (LAYERS, D, HEADS * HEAD), D ** -0.5).astype(jnp.bfloat16),
        'w_k': gaussian(shared_keys[2], (LAYERS, D, KV_HEADS * HEAD), D ** -0.5).astype(jnp.bfloat16),
        'w_v': gaussian(shared_keys[3], (LAYERS, D, KV_HEADS * HEAD), D ** -0.5).astype(jnp.bfloat16),
        'w_o': gaussian(shared_keys[4], (LAYERS, HEADS * HEAD, D), (HEADS * HEAD) ** -0.5).astype(jnp.bfloat16),
        'mlp_gain': jax.random.uniform(shared_keys[5], (LAYERS, D), jnp.float32, 0.5, 1.5).astype(jnp.bfloat16),
        'w_gate': gaussian(shared_keys[6], (LAYERS, D, FF), D ** -0.5).astype(jnp.bfloat16),
        'w_up': gaussian(shared_keys[7], (LAYERS, D, FF), D ** -0.5).astype(jnp.bfloat16),
        'w_down': gaussian(shared_keys[8], (LAYERS, FF, D), 1.5 * FF ** -0.5).astype(jnp.bfloat16),
        'k_cache': k_cache.astype(jnp.bfloat16),
        'v_cache': v_cache.astype(jnp.bfloat16),
    }


def rms_norm(x, norm_gain):
    x_f32 = x.astype(jnp.float32)
    inv_rms = lax.rsqrt(jnp.mean(x_f32 * x_f32, axis=-1, keepdims=True) + EPSILON)
    return (x_f32 * inv_rms * norm_gain.astype(jnp.float32)).astype(jnp.bfloat16)


def rope_tables(positions):
    freq_exps = jnp.arange(0, HEAD, 2, dtype=jnp.float32) / HEAD
    angles = positions.astype(jnp.float32)[:, None] * jnp.power(ROPE_BASE, -freq_exps)[None, :]
    return jnp.cos(angles)[:, None, :], jnp.sin(angles)[:, None, :]


def apply_rope(vectors, cos_tab, sin_tab):
    half_dim = HEAD // 2
    vec_f32 = vectors.astype(jnp.float32)
    first = vec_f32[..., :half_dim]
    second = vec_f32[..., half_dim:]
    return jnp.concatenate([first * cos_tab - second * sin_tab, second * cos_tab + first * sin_tab], axis=-1).astype(jnp.bfloat16)


def decode_row(row_args):
    q_row, k_row, v_row, kc_row, vc_row, length = row_args
    q_f32 = q_row.reshape(KV_HEADS, GROUP, HEAD).astype(jnp.float32)
    logits_cache = jnp.einsum('grd,gsd->grs', q_f32, kc_row.astype(jnp.float32)) * ATTN_SCALE
    logits_cache = jnp.where(jnp.arange(SEQ)[None, None, :] < length, logits_cache, -jnp.inf)
    logits_self = jnp.einsum('grd,gd->gr', q_f32, k_row.astype(jnp.float32))[:, :, None] * ATTN_SCALE
    prob_all = jax.nn.softmax(jnp.concatenate([logits_cache, logits_self], axis=-1), axis=-1)
    prob_all = prob_all.astype(jnp.bfloat16).astype(jnp.float32)
    result = jnp.einsum('grs,gsd->grd', prob_all[..., :SEQ], vc_row.astype(jnp.float32)) + prob_all[..., SEQ:] * v_row.astype(jnp.float32)[:, None, :]
    return result.astype(jnp.bfloat16).reshape(HEADS * HEAD)


def chunk_attention(q_chk, k_chk, v_chk, kc_row, vc_row, prefix_len):
    q_heads = q_chk.reshape(CHUNK, KV_HEADS, GROUP, HEAD).transpose(1, 0, 2, 3)
    k_heads = k_chk.transpose(1, 0, 2)
    v_heads = v_chk.transpose(1, 0, 2)
    cache_mask = jnp.arange(SEQ)[None, None, :] < prefix_len
    tok_ids = jnp.arange(CHUNK)
    causal_mask = (tok_ids[None, :] <= tok_ids[:, None])[:, None, :]

    def one_head(head_args):
        q_head, k_head, v_head, kc_head, vc_head = head_args
        q_f32 = q_head.astype(jnp.float32)
        logits_cache = jnp.einsum('crd,sd->crs', q_f32, kc_head.astype(jnp.float32)) * ATTN_SCALE
        logits_cache = jnp.where(cache_mask, logits_cache, -jnp.inf)
        logits_new = jnp.einsum('crd,jd->crj', q_f32, k_head.astype(jnp.float32)) * ATTN_SCALE
        logits_new = jnp.where(causal_mask, logits_new, -jnp.inf)
        prob_all = jax.nn.softmax(jnp.concatenate([logits_cache, logits_new], axis=-1), axis=-1)
        prob_all = prob_all.astype(jnp.bfloat16).astype(jnp.float32)
        result = jnp.einsum('crs,sd->crd', prob_all[..., :SEQ], vc_head.astype(jnp.float32)) + jnp.einsum('crj,jd->crd', prob_all[..., SEQ:], v_head.astype(jnp.float32))
        return result.astype(jnp.bfloat16)

    heads_out = lax.map(one_head, (q_heads, k_heads, v_heads, kc_row, vc_row))
    return heads_out.transpose(1, 0, 2, 3).reshape(CHUNK, HEADS * HEAD)


def decoder_layer(x, lengths, cos_tab, sin_tab, params):
    attn_gain, w_q, w_k, w_v, w_o, mlp_gain, w_gate, w_up, w_down, k_cache, v_cache = params
    normed = rms_norm(x, attn_gain)
    q_all = apply_rope(jnp.dot(normed, w_q, preferred_element_type=jnp.float32).astype(jnp.bfloat16).reshape(TOKENS, HEADS, HEAD), cos_tab, sin_tab)
    k_all = apply_rope(jnp.dot(normed, w_k, preferred_element_type=jnp.float32).astype(jnp.bfloat16).reshape(TOKENS, KV_HEADS, HEAD), cos_tab, sin_tab)
    v_all = jnp.dot(normed, w_v, preferred_element_type=jnp.float32).astype(jnp.bfloat16).reshape(TOKENS, KV_HEADS, HEAD)
    dec_out = lax.map(decode_row, (q_all[:BATCH], k_all[:BATCH], v_all[:BATCH], k_cache[:BATCH], v_cache[:BATCH], lengths[:BATCH]))
    chk_out = chunk_attention(q_all[BATCH:], k_all[BATCH:], v_all[BATCH:], k_cache[BATCH], v_cache[BATCH], lengths[BATCH])
    attended = jnp.concatenate([dec_out, chk_out], axis=0)
    hidden = (x.astype(jnp.float32) + jnp.dot(attended, w_o, preferred_element_type=jnp.float32)).astype(jnp.bfloat16)
    mlp_in = rms_norm(hidden, mlp_gain)
    gate_proj = jnp.dot(mlp_in, w_gate, preferred_element_type=jnp.float32)
    up_proj = jnp.dot(mlp_in, w_up, preferred_element_type=jnp.float32)
    activated = (jax.nn.silu(gate_proj) * up_proj).astype(jnp.bfloat16)
    down_proj = jnp.dot(activated, w_down, preferred_element_type=jnp.float32)
    return (hidden.astype(jnp.float32) + down_proj).astype(jnp.bfloat16)


def reference(x, lengths, attn_gain, w_q, w_k, w_v, w_o, mlp_gain, w_gate, w_up, w_down, k_cache, v_cache):
    positions = jnp.concatenate([lengths[:BATCH], lengths[BATCH] + jnp.arange(CHUNK, dtype=jnp.int32)])
    cos_tab, sin_tab = rope_tables(positions)

    def layer_step(hidden, params):
        return decoder_layer(hidden, lengths, cos_tab, sin_tab, params), None

    result, unused = lax.scan(layer_step, x, (attn_gain, w_q, w_k, w_v, w_o, mlp_gain, w_gate, w_up, w_down, k_cache, v_cache))
    return result
```

```python
import functools

import jax
import jax.numpy as jnp
from jax import lax
from jax.experimental import pallas as pl
from jax.experimental.pallas import tpu as pltpu
from jax.sharding import PartitionSpec as P

ROPE_BASE = 500000.0
EPSILON = 1e-5
MESH = pl.DeviceIdType.MESH
LANES = 128


def rms_norm(x, norm_gain):
    x_f32 = x.astype(jnp.float32)
    inv_rms = lax.rsqrt(jnp.mean(x_f32 * x_f32, axis=-1, keepdims=True) + EPSILON)
    return (x_f32 * inv_rms * norm_gain.astype(jnp.float32)).astype(jnp.bfloat16)


def rope_tables(positions, head_dim):
    freq_exps = jnp.arange(0, head_dim, 2, dtype=jnp.float32) / head_dim
    angles = positions.astype(jnp.float32)[:, None] * jnp.power(ROPE_BASE, -freq_exps)[None, :]
    return jnp.cos(angles)[:, None, :], jnp.sin(angles)[:, None, :]


def apply_rope(vectors, cos_tab, sin_tab):
    half_dim = vectors.shape[-1] // 2
    vec_f32 = vectors.astype(jnp.float32)
    first = vec_f32[..., :half_dim]
    second = vec_f32[..., half_dim:]
    return jnp.concatenate([first * cos_tab - second * sin_tab, second * cos_tab + first * sin_tab], axis=-1).astype(jnp.bfloat16)


def project(normed, weight, head_dim):
    return jnp.dot(normed, weight, preferred_element_type=jnp.float32).astype(jnp.bfloat16).reshape(normed.shape[0], -1, head_dim)


def attention(q_rot, k_rot, v_new, k_cache, v_cache, lengths):
    dec_rows = lengths.shape[0] - 1
    kv_local = k_cache.shape[1]
    seq_len = k_cache.shape[2]
    head_dim = k_cache.shape[3]
    tok_count = q_rot.shape[0]
    chunk_len = tok_count - dec_rows
    attn_scale = head_dim ** -0.5
    q_grouped = q_rot.reshape(tok_count, kv_local, -1, head_dim)
    q_dec = q_grouped[:dec_rows]
    q_chk = q_grouped[dec_rows:]
    seq_ids = jnp.arange(seq_len)
    dec_cache = jnp.einsum('bgrd,bgsd->bgrs', q_dec, k_cache[:dec_rows], preferred_element_type=jnp.float32) * attn_scale
    dec_cache = jnp.where(seq_ids[None, None, None, :] < lengths[:dec_rows, None, None, None], dec_cache, -jnp.inf)
    dec_self = jnp.einsum('bgrd,bgd->bgr', q_dec, k_rot[:dec_rows], preferred_element_type=jnp.float32)[..., None] * attn_scale
    dec_prob = jax.nn.softmax(jnp.concatenate([dec_cache, dec_self], axis=-1), axis=-1).astype(jnp.bfloat16)
    dec_out = jnp.einsum('bgrs,bgsd->bgrd', dec_prob[..., :seq_len], v_cache[:dec_rows], preferred_element_type=jnp.float32) + dec_prob[..., seq_len:].astype(jnp.float32) * v_new[:dec_rows, :, None, :].astype(jnp.float32)
    chk_cache = jnp.einsum('cgrd,gsd->cgrs', q_chk, k_cache[dec_rows], preferred_element_type=jnp.float32) * attn_scale
    chk_cache = jnp.where(seq_ids[None, None, None, :] < lengths[dec_rows], chk_cache, -jnp.inf)
    chk_self = jnp.einsum('cgrd,jgd->cgrj', q_chk, k_rot[dec_rows:], preferred_element_type=jnp.float32) * attn_scale
    tok_ids = jnp.arange(chunk_len)
    causal_mask = tok_ids[None, :] <= tok_ids[:, None]
    chk_self = jnp.where(causal_mask[:, None, None, :], chk_self, -jnp.inf)
    chk_prob = jax.nn.softmax(jnp.concatenate([chk_cache, chk_self], axis=-1), axis=-1).astype(jnp.bfloat16)
    chk_out = jnp.einsum('cgrs,gsd->cgrd', chk_prob[..., :seq_len], v_cache[dec_rows], preferred_element_type=jnp.float32) + jnp.einsum('cgrj,jgd->cgrd', chk_prob[..., seq_len:], v_new[dec_rows:], preferred_element_type=jnp.float32)
    return jnp.concatenate([dec_out.reshape(dec_rows, -1), chk_out.reshape(chunk_len, -1)], axis=0).astype(jnp.bfloat16)


def sum_kernel(chips, part_ref, x_ref, out_ref, pair_in, pair_sum, ring_in, relay,
               pair_send, pair_recv, ring_send, ring_recv, gather_send, gather_recv, share_send, share_recv):
    me = lax.axis_index('tp')
    core, chip = lax.rem(me, 2), lax.div(me, 2)
    half = part_ref.shape[1] // 2
    width = half // chips
    sub = width // 2

    def at_chip(step):
        return lax.rem(chip + step + chips, chips)

    partner = {'tp': chip * 2 + 1 - core}
    right = {'tp': at_chip(1) * 2 + core}
    left = {'tp': at_chip(-1) * 2 + core}

    def columns(which_core, which_chip, part):
        start = which_core * half + which_chip * width
        if part == 2:
            return pl.ds(pl.multiple_of(start, LANES), width)
        return pl.ds(pl.multiple_of(start + part * sub, LANES), sub)

    def copy(src, dst, send, recv, to):
        return pltpu.make_async_remote_copy(src_ref=src, dst_ref=dst, send_sem=send, recv_sem=recv, device_id=to, device_id_type=MESH)

    barrier = pltpu.get_barrier_semaphore()
    for device in (partner, right, left):
        pl.semaphore_signal(barrier, inc=1, device_id=device, device_id_type=MESH)
    pl.semaphore_wait(barrier, 3)

    steps = (2, 1, -1, 0)
    pairs = []
    for slot, step in enumerate(steps):
        pairs.append(copy(part_ref.at[:, columns(1 - core, at_chip(step), 2)], pair_in.at[slot], pair_send.at[slot], pair_recv.at[slot], partner))
        pairs[-1].start()

    def pair_add(slot):
        pairs[slot].wait_recv()
        own = part_ref[:, columns(core, at_chip(steps[slot]), 2)].astype(jnp.float32)
        return own + pair_in[slot].astype(jnp.float32)

    def ring(src, slot, to):
        ring_copy = copy(src, ring_in.at[slot], ring_send.at[slot], ring_recv.at[slot], to)
        ring_copy.start()
        return ring_copy

    total = pair_add(0).astype(jnp.bfloat16)
    pair_sum[0] = total[:, :sub]
    pair_sum[1] = total[:, sub:]
    rings = [None] * 6
    rings[0] = ring(pair_sum.at[0], 0, right)
    rings[3] = ring(pair_sum.at[1], 3, left)
    ahead = pair_add(1)
    pair_sum[2] = ahead[:, sub:].astype(jnp.bfloat16)
    rings[1] = ring(pair_sum.at[2], 1, right)
    behind = pair_add(2)
    pair_sum[3] = behind[:, :sub].astype(jnp.bfloat16)
    rings[4] = ring(pair_sum.at[3], 4, left)
    rings[0].wait_recv()
    relay[0] = (ahead[:, :sub] + ring_in[0].astype(jnp.float32)).astype(jnp.bfloat16)
    rings[2] = ring(relay.at[0], 2, right)
    rings[3].wait_recv()
    relay[1] = (behind[:, sub:] + ring_in[3].astype(jnp.float32)).astype(jnp.bfloat16)
    rings[5] = ring(relay.at[1], 5, left)
    mine = pair_add(3) + x_ref[:, columns(core, chip, 2)].astype(jnp.float32)
    rings[1].wait_recv()
    rings[4].wait_recv()
    first = mine[:, :sub] + ring_in[4].astype(jnp.float32)
    second = mine[:, sub:] + ring_in[1].astype(jnp.float32)
    rings[2].wait_recv()
    out_ref[:, columns(core, chip, 0)] = (first + ring_in[2].astype(jnp.float32)).astype(jnp.bfloat16)

    def gather(step, part, slot, dst_slot, to):
        block = out_ref.at[:, columns(core, at_chip(step), part)]
        gather_copy = copy(block, block, gather_send.at[slot], gather_recv.at[dst_slot], to)
        gather_copy.start()
        return gather_copy

    def share(step, part, slot):
        block = out_ref.at[:, columns(core, at_chip(step), part)]
        share_copy = copy(block, block, share_send.at[slot], share_recv.at[slot], partner)
        share_copy.start()
        return share_copy

    gathers = [None] * 6
    gathers[0] = gather(0, 0, 0, 0, right)
    rings[5].wait_recv()
    out_ref[:, columns(core, chip, 1)] = (second + ring_in[5].astype(jnp.float32)).astype(jnp.bfloat16)
    gathers[2] = gather(0, 1, 2, 2, left)
    gathers[1] = gather(0, 1, 1, 1, right)
    gathers[3] = gather(0, 0, 3, 3, left)
    shares = [share(0, 2, 0)]
    gathers[0].wait_recv()
    gathers[4] = gather(-1, 0, 4, 4, right)
    shares.append(share(-1, 0, 1))
    gathers[2].wait_recv()
    gathers[5] = gather(1, 1, 5, 5, left)
    shares.append(share(1, 1, 2))
    gathers[1].wait_recv()
    shares.append(share(-1, 1, 3))
    gathers[3].wait_recv()
    shares.append(share(1, 0, 4))
    gathers[4].wait_recv()
    shares.append(share(2, 0, 5))
    gathers[5].wait_recv()
    shares.append(share(2, 1, 6))
    for each in shares:
        each.wait_recv()
    for each in pairs + rings + gathers + shares:
        each.wait_send()


def add_sum(part, x, tp_size, collective_id):
    rows, cols = part.shape
    width = cols // tp_size
    sub = width // 2
    dma = pltpu.SemaphoreType.DMA
    return pl.pallas_call(
        functools.partial(sum_kernel, tp_size // 2),
        out_shape=jax.ShapeDtypeStruct(part.shape, part.dtype),
        in_specs=[pl.BlockSpec(memory_space=pltpu.VMEM)] * 2,
        out_specs=pl.BlockSpec(memory_space=pltpu.VMEM),
        scratch_shapes=[
            pltpu.VMEM((4, rows, width), jnp.bfloat16),
            pltpu.VMEM((4, rows, sub), jnp.bfloat16),
            pltpu.VMEM((6, rows, sub), jnp.bfloat16),
            pltpu.VMEM((2, rows, sub), jnp.bfloat16),
            dma((4,)), dma((4,)), dma((6,)), dma((6,)), dma((6,)), dma((6,)), dma((7,)), dma((7,)),
        ],
        compiler_params=pltpu.CompilerParams(collective_id=collective_id, has_side_effects=True),
    )(part, x)


def decoder_layer(x, cos_tab, sin_tab, lengths, attn_gain, w_q, w_k, w_v, w_o, mlp_gain, w_gate, w_up, w_down, k_cache, v_cache, tp_size, layer_idx):
    head_dim = k_cache.shape[-1]
    normed = rms_norm(x, attn_gain)
    q_rot = apply_rope(project(normed, w_q, head_dim), cos_tab, sin_tab)
    k_rot = apply_rope(project(normed, w_k, head_dim), cos_tab, sin_tab)
    v_new = project(normed, w_v, head_dim)
    attended = attention(q_rot, k_rot, v_new, k_cache, v_cache, lengths)
    attn_part = jnp.dot(attended, w_o, preferred_element_type=jnp.float32).astype(jnp.bfloat16)
    hidden = add_sum(attn_part, x, tp_size, 2 * layer_idx)
    mlp_in = rms_norm(hidden, mlp_gain)
    gate_proj = jnp.dot(mlp_in, w_gate, preferred_element_type=jnp.float32)
    up_proj = jnp.dot(mlp_in, w_up, preferred_element_type=jnp.float32)
    activated = (jax.nn.silu(gate_proj) * up_proj).astype(jnp.bfloat16)
    mlp_part = jnp.dot(activated, w_down, preferred_element_type=jnp.float32).astype(jnp.bfloat16)
    return add_sum(mlp_part, hidden, tp_size, 2 * layer_idx + 1)


def solution(mesh):
    col_spec = P(None, None, 'tp')
    row_spec = P(None, 'tp', None)
    cache_spec = P(None, 'dp', 'tp', None, None)
    in_specs = (P('dp', None), P('dp'), P(), col_spec, col_spec, col_spec, row_spec, P(), col_spec, col_spec, row_spec, cache_spec, cache_spec)
    tp_size = mesh.shape['tp']

    def body(x, lengths, attn_gain, w_q, w_k, w_v, w_o, mlp_gain, w_gate, w_up, w_down, k_cache, v_cache):
        dec_rows = lengths.shape[0] - 1
        chunk_len = x.shape[0] - dec_rows
        positions = jnp.concatenate([lengths[:dec_rows], lengths[dec_rows] + jnp.arange(chunk_len, dtype=jnp.int32)])
        cos_tab, sin_tab = rope_tables(positions, k_cache.shape[-1])
        hidden = x
        for layer_idx in range(w_q.shape[0]):
            hidden = decoder_layer(hidden, cos_tab, sin_tab, lengths, attn_gain[layer_idx], w_q[layer_idx], w_k[layer_idx], w_v[layer_idx], w_o[layer_idx], mlp_gain[layer_idx], w_gate[layer_idx], w_up[layer_idx], w_down[layer_idx], k_cache[layer_idx], v_cache[layer_idx], tp_size, layer_idx)
        return hidden

    return jax.shard_map(body, mesh=mesh, in_specs=in_specs, out_specs=P('dp', None), check_vma=False)
```

```python
import functools

import jax
import jax.numpy as jnp
from jax import lax
from jax.experimental import pallas as pl
from jax.experimental.pallas import tpu as pltpu
from jax.sharding import PartitionSpec as P

ROPE_BASE = 500000.0
EPSILON = 1e-5
MESH = pl.DeviceIdType.MESH
LANES = 128
SEQS = 8
VMEM_LIMIT = 67043328
F32 = jnp.float32
BF16 = jnp.bfloat16
NT = (((1,), (1,)), ((), ()))


def matmul(a, b):
    return jnp.dot(a, b, preferred_element_type=F32)


def matmul_nt(a, b):
    return lax.dot_general(a, b, NT, preferred_element_type=F32)


def layer_kernel(chips, x_ref, lens_ref, freq_ref, again_ref, mgain_ref, wq_hbm, wk_hbm, wv_hbm, wo_hbm, wg_hbm, wu_hbm, wd_hbm, k_hbm, v_hbm,
                 out_ref,
                 wq, wkv, wo, wg, wu, wd, kbuf, vbuf, hid, normed, act, part, lens_v, cos_t, sin_t, q_t, k_t, v_t, self_t, qbd, qh, oh, att,
                 pair_in, pair_sum, ring_in, relay,
                 load_sem, cache_sem, pair_send, pair_recv, ring_send, ring_recv, gather_send, gather_recv, share_send, share_recv):
    layers = wq.shape[0]
    rows, cols = x_ref.shape
    dec = lens_v.shape[0]
    chunk = rows - dec
    head = k_hbm.shape[2]
    seq_len = k_hbm.shape[3]
    scale = head ** -0.5
    groups = dec // SEQS
    half = cols // 2
    width = half // chips
    sub = width // 2

    me = lax.axis_index('tp')
    core, chip = lax.rem(me, 2), lax.div(me, 2)

    def at_chip(step):
        return lax.rem(chip + step + chips, chips)

    partner = {'tp': chip * 2 + 1 - core}
    right = {'tp': at_chip(1) * 2 + core}
    left = {'tp': at_chip(-1) * 2 + core}

    def weight_loads(layer, names):
        table = {
            'q': [(wq_hbm.at[layer], wq.at[layer], 0)],
            'kv': [(wk_hbm.at[layer], wkv.at[layer, 0:head], 1), (wk_hbm.at[layer], wkv.at[layer, head:2 * head], 2),
                   (wv_hbm.at[layer], wkv.at[layer, 2 * head:3 * head], 3), (wv_hbm.at[layer], wkv.at[layer, 3 * head:4 * head], 4)],
            'o': [(wo_hbm.at[layer], wo.at[layer], 5)],
            'g': [(wg_hbm.at[layer], wg.at[layer], 6)],
            'u': [(wu_hbm.at[layer], wu.at[layer], 7)],
            'd': [(wd_hbm.at[layer], wd.at[layer], 8)],
        }
        return [pltpu.make_async_copy(src, dst, load_sem.at[layer, slot]) for name in names for src, dst, slot in table[name]]

    def group_load(layer, which, group):
        src, dst = ((k_hbm, kbuf), (v_hbm, vbuf))[which]
        block = pl.ds(group * SEQS, SEQS)
        return pltpu.make_async_copy(src.at[layer, block], dst.at[block], cache_sem.at[layer, which, group])

    def chunk_load(layer, which):
        src, dst = ((k_hbm, kbuf), (v_hbm, vbuf))[which]
        return pltpu.make_async_copy(src.at[layer, dec], dst.at[dec], cache_sem.at[layer, which, groups])

    def start(copies):
        for each in copies:
            each.start()

    def wait(copies):
        for each in copies:
            each.wait()

    def start_caches(layer):
        start([chunk_load(layer, 0), chunk_load(layer, 1)])

        def issue(group, carry):
            group_load(layer, 0, group).start()
            group_load(layer, 1, group).start()
            return carry

        lax.fori_loop(0, groups, issue, 0)

    start(weight_loads(0, ('q', 'kv')))
    start_caches(0)
    start(weight_loads(0, ('o', 'g', 'u', 'd')))

    barrier = pltpu.get_barrier_semaphore()
    for device in (partner, right, left):
        pl.semaphore_signal(barrier, inc=1, device_id=device, device_id_type=MESH)

    def fill(row, carry):
        lens_v[pl.ds(row, 1), :] = jnp.full((1, LANES), lens_ref[row], jnp.int32)
        return carry

    lax.fori_loop(0, dec, fill, 0)

    def table(row, positions):
        angles = positions.astype(F32) * freq_ref[0:1, :]
        cos_t[pl.ds(row, 8), :] = jnp.cos(angles)
        sin_t[pl.ds(row, 8), :] = jnp.sin(angles)

    def dec_table(i, carry):
        row = pl.multiple_of(i * 8, 8)
        table(row, lens_v[pl.ds(row, 8), :])
        return carry

    def chunk_table(i, carry):
        row = pl.multiple_of(i * 8, 8)
        table(dec + row, lens_ref[dec] + row + lax.broadcasted_iota(jnp.int32, (8, LANES), 0))
        return carry

    lax.fori_loop(0, dec // 8, dec_table, 0)
    lax.fori_loop(0, chunk // 8, chunk_table, 0)

    def normalize(src, gain):
        def block(i, carry):
            band = pl.ds(pl.multiple_of(i * 16, 16), 16)
            values = src[band, :].astype(F32)
            inv = lax.rsqrt(jnp.sum(values * values, axis=1, keepdims=True) * (1.0 / cols) + EPSILON)
            normed[band, :] = (values * inv * gain).astype(BF16)
            return carry

        lax.fori_loop(0, rows // 16, block, 0)

    def rope(values):
        wide = values.shape[1]
        lane = lax.broadcasted_iota(jnp.int32, values.shape, 1)
        turned = jnp.where(lane % head < head // 2, -pltpu.roll(values, wide - head // 2, 1), pltpu.roll(values, head // 2, 1))
        cos, sin = cos_t[...], sin_t[...]
        if wide > LANES:
            cos, sin = jnp.concatenate([cos, cos], axis=1), jnp.concatenate([sin, sin], axis=1)
        return (values * cos + turned * sin).astype(BF16).astype(F32)

    def project(layer):
        q_t[...] = rope(matmul(normed[...], wq[layer]).astype(BF16).astype(F32))
        kv = matmul_nt(normed[...], wkv[layer]).astype(BF16)
        k_t[...] = rope(kv[:, :LANES].astype(F32))
        v_t[...] = kv[:, LANES:].astype(F32)

    def decode_setup():
        lane = lax.broadcasted_iota(jnp.int32, (dec, LANES), 1)
        keys = k_t[0:dec, :]
        for pair in range(2):
            block = q_t[0:dec, pair * LANES:(pair + 1) * LANES]
            swapped = pltpu.roll(block, head, 1)
            product = block * keys
            for side in range(2):
                r = 2 * pair + side
                mine = (lane < head) if side == 0 else (lane >= head)
                self_t[r] = jnp.broadcast_to(jnp.sum(jnp.where(mine, product, 0.0), axis=1, keepdims=True) * scale, (dec, LANES))
                twice = jnp.where(mine, block, swapped)
                wide = jnp.concatenate([twice] * (SEQS * head // LANES), axis=1)
                col = lax.broadcasted_iota(jnp.int32, wide.shape, 1)
                row = lax.broadcasted_iota(jnp.int32, wide.shape, 0)
                qbd[r] = jnp.where(col // head == row % SEQS, wide, 0.0)

    def decode(layer):
        def group_step(group, carry):
            band = pl.ds(pl.multiple_of(group * SEQS, SEQS), SEQS)
            heads = qbd.shape[0]
            queries = qbd[:, band, :].reshape(heads * SEQS, SEQS * head).astype(BF16)
            group_load(layer, 0, group).wait()
            logits = matmul(queries, kbuf[pl.ds(group * SEQS, SEQS)].reshape(SEQS * head, seq_len)) * scale
            logits = logits.reshape(heads, SEQS, seq_len)
            seen = lax.broadcasted_iota(jnp.int32, (SEQS, seq_len), 1) < lens_v[band, 0:1]
            logits = jnp.where(seen[None], logits, -jnp.inf)
            own = self_t[:, band, 0:1]
            top = jnp.maximum(jnp.max(logits, axis=2, keepdims=True), own)
            weights = jnp.exp(logits - top)
            own_weight = jnp.exp(own - top)
            inv = 1.0 / (jnp.sum(weights, axis=2, keepdims=True) + own_weight)
            probs = (weights * inv).astype(BF16).reshape(heads * SEQS, seq_len)
            own_prob = (own_weight * inv).astype(BF16).astype(F32)
            group_load(layer, 1, group).wait()
            mixed = matmul_nt(probs, vbuf[pl.ds(group * SEQS, SEQS)].reshape(SEQS * head, seq_len))
            col = lax.broadcasted_iota(jnp.int32, mixed.shape, 1)
            row = lax.broadcasted_iota(jnp.int32, mixed.shape, 0)
            mixed = jnp.where(col // head == row % SEQS, mixed, 0.0)
            folded = mixed[:, 0:LANES]
            for i in range(1, SEQS * head // LANES):
                folded = folded + mixed[:, i * LANES:(i + 1) * LANES]
            folded = folded + pltpu.roll(folded, head, 1)
            result = folded.reshape(heads, SEQS, LANES) + own_prob * v_t[band, :][None]
            lane = lax.broadcasted_iota(jnp.int32, (SEQS, LANES), 1)
            att[band, 0:LANES] = jnp.where(lane < head, result[0], result[1])
            att[band, LANES:2 * LANES] = jnp.where(lane < head, result[2], result[3])
            return carry

        lax.fori_loop(0, groups, group_step, 0, unroll=2)

    def prefill(layer):
        lane = lax.broadcasted_iota(jnp.int32, (chunk, LANES), 1)
        for pair in range(2):
            block = q_t[dec:rows, pair * LANES:(pair + 1) * LANES]
            qh[2 * pair] = jnp.where(lane < head, block, 0.0).astype(BF16)
            qh[2 * pair + 1] = jnp.where(lane >= head, block, 0.0).astype(BF16)
        wait([chunk_load(layer, 0), chunk_load(layer, 1)])

        def head_step(r, carry):
            queries = qh[r]
            keys = kbuf[dec]
            logits = matmul(queries, jnp.concatenate([keys, keys], axis=0)) * scale
            seen = lax.broadcasted_iota(jnp.int32, (chunk, seq_len), 1) < lens_ref[dec]
            logits = jnp.where(seen, logits, -jnp.inf)
            own = matmul_nt(queries, k_t[dec:rows, :].astype(BF16)) * scale
            causal = lax.broadcasted_iota(jnp.int32, (chunk, chunk), 1) <= lax.broadcasted_iota(jnp.int32, (chunk, chunk), 0)
            own = jnp.where(causal, own, -jnp.inf)
            top = jnp.maximum(jnp.max(logits, axis=1, keepdims=True), jnp.max(own, axis=1, keepdims=True))
            weights = jnp.exp(logits - top)
            own_weights = jnp.exp(own - top)
            inv = 1.0 / (jnp.sum(weights, axis=1, keepdims=True) + jnp.sum(own_weights, axis=1, keepdims=True))
            probs = (weights * inv).astype(BF16)
            own_probs = (own_weights * inv).astype(BF16)
            values = vbuf[dec]
            oh[r] = matmul_nt(probs, jnp.concatenate([values, values], axis=0)) + matmul(own_probs, v_t[dec:rows, :].astype(BF16))
            return carry

        lax.fori_loop(0, qh.shape[0], head_step, 0)
        for pair in range(2):
            att[dec:rows, pair * LANES:(pair + 1) * LANES] = jnp.where(lane < head, oh[2 * pair], oh[2 * pair + 1])

    def copy(src, dst, send, recv, to):
        return pltpu.make_async_remote_copy(src_ref=src, dst_ref=dst, send_sem=send, recv_sem=recv, device_id=to, device_id_type=MESH)

    def step_of(slot):
        high, low = slot // 2, slot % 2
        return 2 - low + high * (1 - 2 * low)

    pending = []

    def sum_over_tp(index, product, base, target):
        def piece_of(which_core, slot):
            return which_core * chips + at_chip(step_of(slot))

        def pair_copy(slot):
            piece = piece_of(1 - core, slot)
            return copy(part.at[piece], pair_in.at[index, slot], pair_send.at[index, slot], pair_recv.at[index, slot], partner)

        def theirs(slot, carry):
            piece = piece_of(1 - core, slot)
            part[piece] = product(piece).astype(BF16)
            pair_copy(slot).start()
            return carry

        def ours(slot, carry):
            piece = piece_of(core, slot)
            part[piece] = product(piece).astype(BF16)
            return carry

        lax.fori_loop(0, 4, theirs, 0)
        lax.fori_loop(0, 4, ours, 0)

        def columns(which_core, which_chip, side):
            begin = which_core * half + which_chip * width
            if side == 2:
                return pl.ds(pl.multiple_of(begin, LANES), width)
            return pl.ds(pl.multiple_of(begin + side * sub, LANES), sub)

        def pair_add(slot):
            pair_copy(slot).wait_recv()
            return part[piece_of(core, slot)].astype(F32) + pair_in[index, slot].astype(F32)

        sent = []

        def ring(src, slot, to):
            ring_copy = copy(src, ring_in.at[index, slot], ring_send.at[index, slot], ring_recv.at[index, slot], to)
            ring_copy.start()
            sent.append(ring_copy)
            return ring_copy

        far = pair_add(0).astype(BF16)
        pair_sum[index, 0] = far[:, :sub]
        pair_sum[index, 1] = far[:, sub:]
        ring0 = ring(pair_sum.at[index, 0], 0, right)
        ring3 = ring(pair_sum.at[index, 1], 3, left)
        ahead = pair_add(1)
        pair_sum[index, 2] = ahead[:, sub:].astype(BF16)
        ring1 = ring(pair_sum.at[index, 2], 1, right)
        behind = pair_add(2)
        pair_sum[index, 3] = behind[:, :sub].astype(BF16)
        ring4 = ring(pair_sum.at[index, 3], 4, left)
        ring0.wait_recv()
        relay[index, 0] = (ahead[:, :sub] + ring_in[index, 0].astype(F32)).astype(BF16)
        ring2 = ring(relay.at[index, 0], 2, right)
        ring3.wait_recv()
        relay[index, 1] = (behind[:, sub:] + ring_in[index, 3].astype(F32)).astype(BF16)
        ring5 = ring(relay.at[index, 1], 5, left)
        mine = pair_add(3) + base[:, columns(core, chip, 2)].astype(F32)
        ring1.wait_recv()
        ring4.wait_recv()
        first = mine[:, :sub] + ring_in[index, 4].astype(F32)
        second = mine[:, sub:] + ring_in[index, 1].astype(F32)
        ring2.wait_recv()
        target[:, columns(core, chip, 0)] = (first + ring_in[index, 2].astype(F32)).astype(BF16)

        def gather(step, side, slot, to):
            block = target.at[:, columns(core, at_chip(step), side)]
            gather_copy = copy(block, block, gather_send.at[index, slot], gather_recv.at[index, slot], to)
            gather_copy.start()
            sent.append(gather_copy)
            return gather_copy

        shares = []

        def share(step, side, slot):
            block = target.at[:, columns(core, at_chip(step), side)]
            share_copy = copy(block, block, share_send.at[index, slot], share_recv.at[index, slot], partner)
            share_copy.start()
            sent.append(share_copy)
            shares.append(share_copy)

        gather0 = gather(0, 0, 0, right)
        ring5.wait_recv()
        target[:, columns(core, chip, 1)] = (second + ring_in[index, 5].astype(F32)).astype(BF16)
        gather2 = gather(0, 1, 2, left)
        gather1 = gather(0, 1, 1, right)
        gather3 = gather(0, 0, 3, left)
        share(0, 2, 0)
        gather0.wait_recv()
        gather4 = gather(-1, 0, 4, right)
        share(-1, 0, 1)
        gather2.wait_recv()
        gather5 = gather(1, 1, 5, left)
        share(1, 1, 2)
        gather1.wait_recv()
        share(-1, 1, 3)
        gather3.wait_recv()
        share(1, 0, 4)
        gather4.wait_recv()
        share(2, 0, 5)
        gather5.wait_recv()
        share(2, 1, 6)
        for each in shares:
            each.wait_recv()
        for slot in range(4):
            pair_copy(slot).wait_send()
        for each in sent:
            each.wait_send()

    def piece_columns(piece):
        return pl.ds(pl.multiple_of(piece * width, LANES), width)

    residual = x_ref
    for layer in range(layers):
        normalize(residual, again_ref[...].astype(F32)[layer:layer + 1])
        wait(weight_loads(layer, ('q', 'kv')))
        project(layer)
        decode_setup()
        decode(layer)
        prefill(layer)
        if layer + 1 < layers:
            start_caches(layer + 1)
            start(weight_loads(layer + 1, ('q', 'kv', 'o', 'g', 'u', 'd')))
        if layer == 0:
            pl.semaphore_wait(barrier, 3)
        wait(weight_loads(layer, ('o',)))
        sum_over_tp(2 * layer, lambda piece: matmul(att[...].astype(BF16), wo[layer, :, piece_columns(piece)]), residual, hid.at[2 * layer])
        residual = hid.at[2 * layer]
        normalize(residual, mgain_ref[...].astype(F32)[layer:layer + 1])
        wait(weight_loads(layer, ('g', 'u')))

        def mlp_step(i, carry):
            piece = piece_columns(i)
            gate = matmul(normed[...], wg[layer, :, piece])
            up = matmul(normed[...], wu[layer, :, piece])
            act[:, piece] = (gate / (1.0 + jnp.exp(-gate)) * up).astype(BF16)
            return carry

        lax.fori_loop(0, act.shape[1] // width, mlp_step, 0)
        wait(weight_loads(layer, ('d',)))
        target = out_ref if layer + 1 == layers else hid.at[2 * layer + 1]
        sum_over_tp(2 * layer + 1, lambda piece: matmul(act[...], wd[layer, :, piece_columns(piece)]), residual, target)
        residual = target


def run_layers(x, lengths, attn_gain, w_q, w_k, w_v, w_o, mlp_gain, w_gate, w_up, w_down, k_cache, v_cache, tp_size):
    rows, cols = x.shape
    layers = w_q.shape[0]
    head = k_cache.shape[-1]
    seqs, seq_len = k_cache.shape[1], k_cache.shape[3]
    dec = seqs - 1
    chunk = rows - dec
    heads = w_q.shape[2] // head
    inner = w_gate.shape[2]
    width = cols // tp_size
    sub = width // 2
    sums = 2 * layers
    freq = jnp.power(ROPE_BASE, -jnp.arange(0, head, 2, dtype=F32) / head)
    freq = jnp.broadcast_to(jnp.tile(freq, LANES // (head // 2))[None], (8, LANES))
    turned = lambda array: jnp.swapaxes(array, -1, -2)
    k_cols, v_cols = turned(k_cache)[:, :, 0], turned(v_cache)[:, :, 0]
    dma = pltpu.SemaphoreType.DMA
    vmem = pl.BlockSpec(memory_space=pltpu.VMEM)
    hbm = pl.BlockSpec(memory_space=pl.ANY)
    scratch = [
        ((layers, cols, heads * head), BF16), ((layers, 4 * head, cols), BF16), ((layers, heads * head, cols), BF16),
        ((layers, cols, inner), BF16), ((layers, cols, inner), BF16), ((layers, inner, cols), BF16),
        ((seqs, head, seq_len), BF16), ((seqs, head, seq_len), BF16),
        ((sums - 1, rows, cols), BF16), ((rows, cols), BF16), ((rows, inner), BF16), ((tp_size, rows, width), BF16),
        ((dec, LANES), jnp.int32), ((rows, LANES), F32), ((rows, LANES), F32),
        ((rows, heads * head), F32), ((rows, LANES), F32), ((rows, LANES), F32),
        ((heads, dec, LANES), F32), ((heads, dec, SEQS * head), F32), ((heads, chunk, LANES), BF16), ((heads, chunk, LANES), F32),
        ((rows, heads * head), F32),
        ((sums, 4, rows, width), BF16), ((sums, 4, rows, sub), BF16), ((sums, 6, rows, sub), BF16), ((sums, 2, rows, sub), BF16),
    ]
    semaphores = [(layers, 9), (layers, 2, dec // SEQS + 1), (sums, 4), (sums, 4), (sums, 6), (sums, 6), (sums, 6), (sums, 6), (sums, 7), (sums, 7)]
    return pl.pallas_call(
        functools.partial(layer_kernel, tp_size // 2),
        out_shape=jax.ShapeDtypeStruct(x.shape, x.dtype),
        in_specs=[vmem, pl.BlockSpec(memory_space=pltpu.SMEM), vmem, vmem, vmem] + [hbm] * 9,
        out_specs=vmem,
        scratch_shapes=[pltpu.VMEM(shape, dtype) for shape, dtype in scratch] + [dma(shape) for shape in semaphores],
        compiler_params=pltpu.CompilerParams(collective_id=0, has_side_effects=True, vmem_limit_bytes=VMEM_LIMIT),
    )(x, lengths, freq, attn_gain, mlp_gain, w_q, turned(w_k), turned(w_v), w_o, w_gate, w_up, w_down, k_cols, v_cols)


def solution(mesh):
    col_spec = P(None, None, 'tp')
    row_spec = P(None, 'tp', None)
    cache_spec = P(None, 'dp', 'tp', None, None)
    in_specs = (P('dp', None), P('dp'), P(), col_spec, col_spec, col_spec, row_spec, P(), col_spec, col_spec, row_spec, cache_spec, cache_spec)
    body = functools.partial(run_layers, tp_size=mesh.shape['tp'])
    return jax.shard_map(body, mesh=mesh, in_specs=in_specs, out_specs=P('dp', None), check_vma=False)
```

```python
import functools

import jax
import jax.numpy as jnp
from jax import lax
from jax.experimental import pallas as pl
from jax.experimental.pallas import tpu as pltpu
from jax.sharding import PartitionSpec as P

ROPE_BASE = 500000.0
EPSILON = 1e-5
MESH = pl.DeviceIdType.MESH
LANES = 128
SEQS = 8
CACHE_LOADS = 4
NEAR_WAIT, NEAR_WIRE, FAR_WAIT, FAR_WIRE = 2.6, 2.1, 3.4, 4.2
VMEM_LIMIT = 67043328
F32 = jnp.float32
BF16 = jnp.bfloat16
NT = (((1,), (1,)), ((), ()))


def matmul(a, b):
    return jnp.dot(a, b, preferred_element_type=F32)


def matmul_nt(a, b):
    return lax.dot_general(a, b, NT, preferred_element_type=F32)


def run_streams(streams):
    now, ready = 0.0, [0.0] * len(streams)
    live = set(range(len(streams)))
    while live:
        pick = min(sorted(live), key=lambda i: ready[i])
        now = max(now, ready[pick])
        try:
            busy, wait = next(streams[pick])
        except StopIteration:
            live.discard(pick)
            continue
        now += busy
        ready[pick] = now + wait


def layer_kernel(chips, x_ref, lens_ref, freq_ref, again_ref, mgain_ref, wq_hbm, wk_hbm, wv_hbm, wo_hbm, wg_hbm, wu_hbm, wd_hbm, k_hbm, v_hbm,
                 out_ref,
                 wq, wkv, wo, wg, wu, wd, kbuf, vbuf, hid, normed, act, lens_v, cos_t, sin_t, q_t, k_t, v_t, self_t, qbd, qh, oh, att,
                 part_a, pair_in_a, pair_sum_a, ring_in_a, part_b, pair_in_b, pair_sum_b, ring_in_b,
                 load_sem, cache_sem, pair_send, pair_recv, ring_send, ring_recv, gather_send, gather_recv, share_send, share_recv):
    layers = wq.shape[0]
    rows, cols = x_ref.shape
    dec = lens_v.shape[0]
    chunk = rows - dec
    head = k_hbm.shape[2]
    seq_len = k_hbm.shape[3]
    heads = qbd.shape[0]
    scale = head ** -0.5
    loads = cache_sem.shape[2] - 1
    load_seqs = dec // loads
    half = cols // 2
    width = half // chips
    span = (slice(0, dec), slice(dec, rows))
    parts = (part_a, part_b)
    buffers = ((pair_in_a, pair_sum_a, ring_in_a), (pair_in_b, pair_sum_b, ring_in_b))

    me = lax.axis_index('tp')
    core, chip = lax.rem(me, 2), lax.div(me, 2)

    def at_chip(step):
        return lax.rem(chip + step + chips, chips)

    partner = {'tp': chip * 2 + 1 - core}
    right = {'tp': at_chip(1) * 2 + core}
    left = {'tp': at_chip(-1) * 2 + core}
    far = {'tp': at_chip(2) * 2 + core}
    others = (far, right, left)

    def load(layer, name):
        src, dst, slot = {
            'q': (wq_hbm.at[layer], wq.at[layer], 0),
            'k0': (wk_hbm.at[layer], wkv.at[layer, 0:head], 1),
            'k1': (wk_hbm.at[layer], wkv.at[layer, head:2 * head], 2),
            'v0': (wv_hbm.at[layer], wkv.at[layer, 2 * head:3 * head], 3),
            'v1': (wv_hbm.at[layer], wkv.at[layer, 3 * head:4 * head], 4),
            'o': (wo_hbm.at[layer], wo.at[layer], 5),
            'g': (wg_hbm.at[layer], wg.at[layer], 6),
            'u': (wu_hbm.at[layer], wu.at[layer], 7),
            'd': (wd_hbm.at[layer], wd.at[layer], 8),
        }[name]
        return pltpu.make_async_copy(src, dst, load_sem.at[layer, slot])

    def cache_load(layer, which, index):
        src, dst = ((k_hbm, kbuf), (v_hbm, vbuf))[which]
        block = pl.ds(index * load_seqs, load_seqs) if index < loads else dec
        return pltpu.make_async_copy(src.at[layer, block], dst.at[block], cache_sem.at[layer, which, index])

    landed = set()

    def arrive(layer, names):
        for name in names:
            if (layer, name) not in landed:
                landed.add((layer, name))
                load(layer, name).wait()

    def arrive_cache(layer, index):
        for which in range(2):
            cache_load(layer, which, index).wait()

    def start(layer, names):
        for name in names:
            load(layer, name).start()

    def start_cache(layer, indices):
        for index in indices:
            for which in range(2):
                cache_load(layer, which, index).start()

    projections = ('q', 'k0', 'k1', 'v0', 'v1')
    start(0, projections)
    start_cache(0, [loads])
    start(0, ('o',))
    start_cache(0, range(loads))
    start(0, ('g', 'u', 'd'))

    barrier = pltpu.get_barrier_semaphore()
    for device in (partner, right, left, far):
        pl.semaphore_signal(barrier, inc=1, device_id=device, device_id_type=MESH)

    def fill(row, carry):
        lens_v[pl.ds(row, 1), :] = jnp.full((1, LANES), lens_ref[row], jnp.int32)
        return carry

    lax.fori_loop(0, dec, fill, 0)

    def table(row, positions):
        angles = positions.astype(F32) * freq_ref[0:1, :]
        cos_t[pl.ds(row, 8), :] = jnp.cos(angles)
        sin_t[pl.ds(row, 8), :] = jnp.sin(angles)

    def dec_table(i, carry):
        row = pl.multiple_of(i * 8, 8)
        table(row, lens_v[pl.ds(row, 8), :])
        return carry

    def chunk_table(i, carry):
        row = pl.multiple_of(i * 8, 8)
        table(dec + row, lens_ref[dec] + row + lax.broadcasted_iota(jnp.int32, (8, LANES), 0))
        return carry

    lax.fori_loop(0, dec // 8, dec_table, 0)
    lax.fori_loop(0, chunk // 8, chunk_table, 0)

    def normalize(stream, src, gain):
        first, last = span[stream].start, span[stream].stop

        def block(i, carry):
            band = pl.ds(pl.multiple_of(first + i * 16, 16), 16)
            values = src[band, :].astype(F32)
            inv = lax.rsqrt(jnp.sum(values * values, axis=1, keepdims=True) * (1.0 / cols) + EPSILON)
            normed[band, :] = (values * inv * gain).astype(BF16)
            return carry

        lax.fori_loop(0, (last - first) // 16, block, 0, unroll=4)

    def rope(stream, values):
        wide = values.shape[1]
        lane = lax.broadcasted_iota(jnp.int32, values.shape, 1)
        turned = jnp.where(lane % head < head // 2, -pltpu.roll(values, wide - head // 2, 1), pltpu.roll(values, head // 2, 1))
        cos, sin = cos_t[span[stream], :], sin_t[span[stream], :]
        if wide > LANES:
            cos, sin = jnp.concatenate([cos, cos], axis=1), jnp.concatenate([sin, sin], axis=1)
        return (values * cos + turned * sin).astype(BF16).astype(F32)

    def project(stream, layer):
        values = normed[span[stream], :]
        q_t[span[stream], :] = rope(stream, matmul(values, wq[layer]).astype(BF16).astype(F32))
        kv = matmul_nt(values, wkv[layer]).astype(BF16)
        k_t[span[stream], :] = rope(stream, kv[:, :LANES].astype(F32))
        v_t[span[stream], :] = kv[:, LANES:].astype(F32)

    def decode_setup():
        lane = lax.broadcasted_iota(jnp.int32, (dec, LANES), 1)
        keys = k_t[0:dec, :]
        for pair in range(heads // 2):
            block = q_t[0:dec, pair * LANES:(pair + 1) * LANES]
            swapped = pltpu.roll(block, head, 1)
            product = block * keys
            for side in range(2):
                r = 2 * pair + side
                mine = (lane < head) if side == 0 else (lane >= head)
                self_t[r] = jnp.broadcast_to(jnp.sum(jnp.where(mine, product, 0.0), axis=1, keepdims=True) * scale, (dec, LANES))
                twice = jnp.where(mine, block, swapped)
                wide = jnp.concatenate([twice] * (SEQS * head // LANES), axis=1)
                col = lax.broadcasted_iota(jnp.int32, wide.shape, 1)
                row = lax.broadcasted_iota(jnp.int32, wide.shape, 0)
                qbd[r] = jnp.where(col // head == row % SEQS, wide, 0.0)

    def decode(bands):
        probs, own_probs = [], []
        for first in bands:
            band = slice(first, first + SEQS)
            queries = qbd[:, band, :].reshape(heads * SEQS, SEQS * head).astype(BF16)
            logits = matmul(queries, kbuf[band].reshape(SEQS * head, seq_len)) * scale
            logits = logits.reshape(heads, SEQS, seq_len)
            seen = lax.broadcasted_iota(jnp.int32, (SEQS, seq_len), 1) < lens_v[band, 0:1]
            logits = jnp.where(seen[None], logits, -jnp.inf)
            own = self_t[:, band, 0:1]
            top = jnp.maximum(jnp.max(logits, axis=2, keepdims=True), own)
            weights = jnp.exp(logits - top)
            own_weight = jnp.exp(own - top)
            inv = 1.0 / (jnp.sum(weights, axis=2, keepdims=True) + own_weight)
            probs.append((weights * inv).astype(BF16).reshape(heads * SEQS, seq_len))
            own_probs.append((own_weight * inv).astype(BF16).astype(F32))
        for first, prob, own_prob in zip(bands, probs, own_probs):
            band = slice(first, first + SEQS)
            mixed = matmul_nt(prob, vbuf[band].reshape(SEQS * head, seq_len))
            col = lax.broadcasted_iota(jnp.int32, mixed.shape, 1)
            row = lax.broadcasted_iota(jnp.int32, mixed.shape, 0)
            mixed = jnp.where(col // head == row % SEQS, mixed, 0.0)
            folded = mixed[:, 0:LANES]
            for i in range(1, SEQS * head // LANES):
                folded = folded + mixed[:, i * LANES:(i + 1) * LANES]
            folded = folded + pltpu.roll(folded, head, 1)
            result = folded.reshape(heads, SEQS, LANES) + own_prob * v_t[band, :][None]
            lane = lax.broadcasted_iota(jnp.int32, (SEQS, LANES), 1)
            att[band, 0:LANES] = jnp.where(lane < head, result[0], result[1])
            att[band, LANES:2 * LANES] = jnp.where(lane < head, result[2], result[3])

    def prefill_setup():
        lane = lax.broadcasted_iota(jnp.int32, (chunk, LANES), 1)
        for pair in range(heads // 2):
            block = q_t[dec:rows, pair * LANES:(pair + 1) * LANES]
            qh[2 * pair] = jnp.where(lane < head, block, 0.0).astype(BF16)
            qh[2 * pair + 1] = jnp.where(lane >= head, block, 0.0).astype(BF16)

    def prefill(r):
        queries = qh[r]
        keys = kbuf[dec]
        logits = matmul(queries, jnp.concatenate([keys, keys], axis=0)) * scale
        seen = lax.broadcasted_iota(jnp.int32, (chunk, seq_len), 1) < lens_ref[dec]
        logits = jnp.where(seen, logits, -jnp.inf)
        own = matmul_nt(queries, k_t[dec:rows, :].astype(BF16)) * scale
        causal = lax.broadcasted_iota(jnp.int32, (chunk, chunk), 1) <= lax.broadcasted_iota(jnp.int32, (chunk, chunk), 0)
        own = jnp.where(causal, own, -jnp.inf)
        top = jnp.maximum(jnp.max(logits, axis=1, keepdims=True), jnp.max(own, axis=1, keepdims=True))
        weights = jnp.exp(logits - top)
        own_weights = jnp.exp(own - top)
        inv = 1.0 / (jnp.sum(weights, axis=1, keepdims=True) + jnp.sum(own_weights, axis=1, keepdims=True))
        probs = (weights * inv).astype(BF16)
        own_probs = (own_weights * inv).astype(BF16)
        values = vbuf[dec]
        oh[r] = matmul_nt(probs, jnp.concatenate([values, values], axis=0)) + matmul(own_probs, v_t[dec:rows, :].astype(BF16))

    def prefill_end():
        lane = lax.broadcasted_iota(jnp.int32, (chunk, LANES), 1)
        for pair in range(heads // 2):
            att[dec:rows, pair * LANES:(pair + 1) * LANES] = jnp.where(lane < head, oh[2 * pair], oh[2 * pair + 1])

    def copy(src, dst, send, recv, to):
        return pltpu.make_async_remote_copy(src_ref=src, dst_ref=dst, send_sem=send, recv_sem=recv, device_id=to, device_id_type=MESH)

    def step_of(slot):
        high, low = slot // 2, slot % 2
        return 2 - low + high * (1 - 2 * low)

    greeted = []

    def sum_over_tp(stream, index, product, product_time, base, target):
        part = parts[stream]
        pair_in, pair_sum, ring_in = buffers[stream]
        band = span[stream]
        sems = index * 2 + stream
        scale_wire = (band.stop - band.start) / rows

        def piece_of(which_core, slot):
            return which_core * chips + at_chip(step_of(slot))

        def pair_copy(slot):
            return copy(part.at[piece_of(1 - core, slot)], pair_in.at[index, slot], pair_send.at[sems, slot], pair_recv.at[sems, slot], partner)

        def theirs(slot):
            piece = piece_of(1 - core, slot)
            part[piece] = product(piece).astype(BF16)

        def ours(slot):
            piece = piece_of(core, slot)
            part[piece] = product(piece).astype(BF16)

        if not greeted:
            greeted.append(True)
            pl.semaphore_wait(barrier, 4)
        for slot in range(4):
            theirs(slot)
        for slot in range(4):
            pair_copy(slot).start()
        for slot in range(4):
            ours(slot)
        yield product_time, 1.1 + 0.3 * scale_wire

        def columns(which_core, which_chip):
            return pl.ds(pl.multiple_of(which_core * half + which_chip * width, LANES), width)

        def pair_add(slot):
            return part[piece_of(core, slot)].astype(F32) + pair_in[index, slot].astype(F32)

        def scatter(slot):
            return copy(pair_sum.at[index, slot], ring_in.at[index, slot], ring_send.at[sems, slot], ring_recv.at[sems, slot], others[slot])

        def gather(slot):
            block = target.at[band, columns(core, chip)]
            return copy(block, block, gather_send.at[sems, slot], gather_recv.at[sems, slot], others[slot])

        def share(step, slot):
            block = target.at[band, columns(core, at_chip(step))]
            return copy(block, block, share_send.at[sems, slot], share_recv.at[sems, slot], partner)

        for slot in range(3):
            pair_copy(slot).wait_recv()
            pair_sum[index, slot] = pair_add(slot).astype(BF16)
            scatter(slot).start()
        yield 0.25, FAR_WAIT + FAR_WIRE * scale_wire
        pair_copy(3).wait_recv()
        total = pair_add(3) + base[band, columns(core, chip)].astype(F32)
        for slot in (1, 2, 0):
            scatter(slot).wait_recv()
            total = total + ring_in[index, slot].astype(F32)
        target[band, columns(core, chip)] = total.astype(BF16)
        for slot in range(3):
            gather(slot).start()
        share(0, 3).start()
        yield 0.25, NEAR_WAIT + NEAR_WIRE * scale_wire
        for slot, step in ((1, -1), (2, 1)):
            gather(slot).wait_recv()
            share(step, slot).start()
        yield 0.05, FAR_WAIT - NEAR_WAIT + (FAR_WIRE - NEAR_WIRE) * scale_wire
        gather(0).wait_recv()
        share(2, 0).start()
        yield 0.05, 1.0 + 0.2 * scale_wire
        for slot in range(4):
            share(0, slot).wait_recv()
        for slot in range(4):
            pair_copy(slot).wait_send()
            share(0, slot).wait_send()
        for slot in range(3):
            scatter(slot).wait_send()
            gather(slot).wait_send()

    def piece_columns(piece):
        return pl.ds(pl.multiple_of(piece * width, LANES), width)

    attended = [0] * layers

    def attention_done(layer):
        attended[layer] += 1
        if attended[layer] == 2 and layer + 1 < layers:
            start(layer + 1, projections)
            start_cache(layer + 1, [loads])
            start(layer + 1, ('o',))
            start_cache(layer + 1, range(loads))
            start(layer + 1, ('g', 'u', 'd'))

    def stream_steps(stream):
        band = span[stream]
        residual = x_ref
        for layer in range(layers):
            normalize(stream, residual, again_ref[...].astype(F32)[layer:layer + 1])
            yield 0.3, 0.0
            arrive(layer, projections)
            project(stream, layer)
            if stream == 0:
                decode_setup()
                yield 1.0, 0.0
                for index in range(loads):
                    arrive_cache(layer, index)
                    decode(range(index * load_seqs, (index + 1) * load_seqs, SEQS))
                    yield 1.4, 0.0
            else:
                prefill_setup()
                yield 0.8, 0.0
                arrive_cache(layer, loads)
                for r in range(heads):
                    prefill(r)
                    yield 0.55, 0.0
                prefill_end()
            attention_done(layer)
            arrive(layer, ('o',))
            target = hid.at[2 * layer]
            yield from sum_over_tp(stream, 2 * layer, lambda piece: matmul(att[band, :].astype(BF16), wo[layer, :, piece_columns(piece)]), 0.3, residual, target)
            residual = target
            normalize(stream, residual, mgain_ref[...].astype(F32)[layer:layer + 1])
            arrive(layer, ('g', 'u'))

            def mlp_step(i, carry):
                piece = piece_columns(i)
                gate = matmul(normed[band, :], wg[layer, :, piece])
                up = matmul(normed[band, :], wu[layer, :, piece])
                act[band, piece] = (gate / (1.0 + jnp.exp(-gate)) * up).astype(BF16)
                return carry

            lax.fori_loop(0, act.shape[1] // width, mlp_step, 0, unroll=2)
            yield 1.4, 0.0
            arrive(layer, ('d',))
            target = out_ref if layer + 1 == layers else hid.at[2 * layer + 1]
            yield from sum_over_tp(stream, 2 * layer + 1, lambda piece: matmul(act[band, :], wd[layer, :, piece_columns(piece)]), 0.6, residual, target)
            residual = target

    run_streams([stream_steps(1), stream_steps(0)])


def run_layers(x, lengths, attn_gain, w_q, w_k, w_v, w_o, mlp_gain, w_gate, w_up, w_down, k_cache, v_cache, tp_size):
    rows, cols = x.shape
    layers = w_q.shape[0]
    head = k_cache.shape[-1]
    seqs, seq_len = k_cache.shape[1], k_cache.shape[3]
    dec = seqs - 1
    chunk = rows - dec
    heads = w_q.shape[2] // head
    inner = w_gate.shape[2]
    width = cols // tp_size
    sums = 2 * layers
    freq = jnp.power(ROPE_BASE, -jnp.arange(0, head, 2, dtype=F32) / head)
    freq = jnp.broadcast_to(jnp.tile(freq, LANES // (head // 2))[None], (8, LANES))
    turned = lambda array: jnp.swapaxes(array, -1, -2)
    k_cols, v_cols = turned(k_cache)[:, :, 0], turned(v_cache)[:, :, 0]
    dma = pltpu.SemaphoreType.DMA
    vmem = pl.BlockSpec(memory_space=pltpu.VMEM)
    hbm = pl.BlockSpec(memory_space=pl.ANY)
    scratch = [
        ((layers, cols, heads * head), BF16), ((layers, 4 * head, cols), BF16), ((layers, heads * head, cols), BF16),
        ((layers, cols, inner), BF16), ((layers, cols, inner), BF16), ((layers, inner, cols), BF16),
        ((seqs, head, seq_len), BF16), ((seqs, head, seq_len), BF16),
        ((sums - 1, rows, cols), BF16), ((rows, cols), BF16), ((rows, inner), BF16),
        ((dec, LANES), jnp.int32), ((rows, LANES), F32), ((rows, LANES), F32),
        ((rows, heads * head), F32), ((rows, LANES), F32), ((rows, LANES), F32),
        ((heads, dec, LANES), F32), ((heads, dec, SEQS * head), F32), ((heads, chunk, LANES), BF16), ((heads, chunk, LANES), F32),
        ((rows, heads * head), F32),
    ]
    for band in (dec, chunk):
        scratch += [((tp_size, band, width), BF16), ((sums, 4, band, width), BF16), ((sums, 3, band, width), BF16), ((sums, 3, band, width), BF16)]
    semaphores = [(layers, 9), (layers, 2, CACHE_LOADS + 1)] + [(2 * sums, count) for count in (4, 4, 3, 3, 3, 3, 4, 4)]
    return pl.pallas_call(
        functools.partial(layer_kernel, tp_size // 2),
        out_shape=jax.ShapeDtypeStruct(x.shape, x.dtype),
        in_specs=[vmem, pl.BlockSpec(memory_space=pltpu.SMEM), vmem, vmem, vmem] + [hbm] * 9,
        out_specs=vmem,
        scratch_shapes=[pltpu.VMEM(shape, dtype) for shape, dtype in scratch] + [dma(shape) for shape in semaphores],
        compiler_params=pltpu.CompilerParams(collective_id=0, has_side_effects=True, vmem_limit_bytes=VMEM_LIMIT),
    )(x, lengths, freq, attn_gain, mlp_gain, w_q, turned(w_k), turned(w_v), w_o, w_gate, w_up, w_down, k_cols, v_cols)


def solution(mesh):
    col_spec = P(None, None, 'tp')
    row_spec = P(None, 'tp', None)
    cache_spec = P(None, 'dp', 'tp', None, None)
    in_specs = (P('dp', None), P('dp'), P(), col_spec, col_spec, col_spec, row_spec, P(), col_spec, col_spec, row_spec, cache_spec, cache_spec)
    body = functools.partial(run_layers, tp_size=mesh.shape['tp'])
    return jax.shard_map(body, mesh=mesh, in_specs=in_specs, out_specs=P('dp', None), check_vma=False)
```

```python
import functools

import jax
import jax.numpy as jnp
from jax import lax
from jax.experimental import pallas as pl
from jax.experimental.pallas import tpu as pltpu
from jax.sharding import PartitionSpec as P

ROPE_BASE = 500000.0
EPSILON = 1e-5
MESH = pl.DeviceIdType.MESH
LANES = 128
SEQS = 8
CACHE_LOADS = 4
NEAR_WAIT, NEAR_WIRE, FAR_WAIT, FAR_WIRE = 2.6, 2.1, 3.4, 4.2
VMEM_LIMIT = 67043328
F32 = jnp.float32
BF16 = jnp.bfloat16
NT = (((1,), (1,)), ((), ()))


def matmul(a, b):
    return jnp.dot(a, b, preferred_element_type=F32)


def matmul_nt(a, b):
    return lax.dot_general(a, b, NT, preferred_element_type=F32)


def run_streams(streams):
    now, ready = 0.0, [0.0] * len(streams)
    arrived = [False] * len(streams)
    live = set(range(len(streams)))

    def order(i):
        return (0, 0, ready[i]) if ready[i] <= now and arrived[i] else (0, 1, i) if ready[i] <= now else (1, ready[i], i)

    while live:
        pick = min(sorted(live), key=order)
        now = max(now, ready[pick])
        try:
            busy, wait = next(streams[pick])
        except StopIteration:
            live.discard(pick)
            continue
        now += busy
        ready[pick] = now + wait
        arrived[pick] = wait > 0


def layer_kernel(chips, x_ref, lens_ref, freq_ref, again_ref, mgain_ref, wq_hbm, wk_hbm, wv_hbm, wo_hbm, wg_hbm, wu_hbm, wd_hbm, k_hbm, v_hbm,
                 out_ref,
                 wq, wkv, wo, wg, wu, wd, kbuf, vbuf, hid, normed, act, lens_v, cos_t, sin_t, q_t, k_t, v_t, self_t, qbd, qh, oh, att,
                 part_a, pair_in_a, pair_sum_a, ring_in_a, part_b, pair_in_b, pair_sum_b, ring_in_b,
                 load_sem, cache_sem, pair_send, pair_recv, ring_send, ring_recv, gather_send, gather_recv, share_send, share_recv):
    layers = wq.shape[0]
    rows, cols = x_ref.shape
    dec = lens_v.shape[0]
    chunk = rows - dec
    head = k_hbm.shape[2]
    seq_len = k_hbm.shape[3]
    heads = qbd.shape[0]
    scale = head ** -0.5
    loads = cache_sem.shape[2] - 1
    load_seqs = dec // loads
    half = cols // 2
    width = half // chips
    span = (slice(0, dec), slice(dec, rows))
    parts = (part_a, part_b)
    buffers = ((pair_in_a, pair_sum_a, ring_in_a), (pair_in_b, pair_sum_b, ring_in_b))

    me = lax.axis_index('tp')
    core, chip = lax.rem(me, 2), lax.div(me, 2)

    def at_chip(step):
        return lax.rem(chip + step + chips, chips)

    partner = {'tp': chip * 2 + 1 - core}
    right = {'tp': at_chip(1) * 2 + core}
    left = {'tp': at_chip(-1) * 2 + core}
    far = {'tp': at_chip(2) * 2 + core}
    others = (far, right, left)

    def load(layer, name):
        src, dst, slot = {
            'q': (wq_hbm.at[layer], wq.at[layer], 0),
            'k0': (wk_hbm.at[layer], wkv.at[layer, 0:head], 1),
            'k1': (wk_hbm.at[layer], wkv.at[layer, head:2 * head], 2),
            'v0': (wv_hbm.at[layer], wkv.at[layer, 2 * head:3 * head], 3),
            'v1': (wv_hbm.at[layer], wkv.at[layer, 3 * head:4 * head], 4),
            'o': (wo_hbm.at[layer], wo.at[layer], 5),
            'g': (wg_hbm.at[layer], wg.at[layer], 6),
            'u': (wu_hbm.at[layer], wu.at[layer], 7),
            'd': (wd_hbm.at[layer], wd.at[layer], 8),
        }[name]
        return pltpu.make_async_copy(src, dst, load_sem.at[layer, slot])

    def cache_load(layer, which, index):
        src, dst = ((k_hbm, kbuf), (v_hbm, vbuf))[which]
        block = pl.ds(index * load_seqs, load_seqs) if index < loads else dec
        return pltpu.make_async_copy(src.at[layer, block], dst.at[block], cache_sem.at[layer, which, index])

    landed = set()

    def arrive(layer, names):
        for name in names:
            if (layer, name) not in landed:
                landed.add((layer, name))
                load(layer, name).wait()

    def arrive_cache(layer, index):
        for which in range(2):
            cache_load(layer, which, index).wait()

    def start(layer, names):
        for name in names:
            load(layer, name).start()

    def start_cache(layer, indices):
        for index in indices:
            for which in range(2):
                cache_load(layer, which, index).start()

    projections = ('q', 'k0', 'k1', 'v0', 'v1')
    start(0, projections)
    start_cache(0, [loads])
    start(0, ('o',))

    barrier = pltpu.get_barrier_semaphore()
    for device in (partner, right, left, far):
        pl.semaphore_signal(barrier, inc=1, device_id=device, device_id_type=MESH)

    def fill(row, carry):
        lens_v[pl.ds(row, 1), :] = jnp.full((1, LANES), lens_ref[row], jnp.int32)
        return carry

    lax.fori_loop(0, dec, fill, 0)

    def table(row, positions):
        angles = positions.astype(F32) * freq_ref[0:1, :]
        cos_t[pl.ds(row, 8), :] = jnp.cos(angles)
        sin_t[pl.ds(row, 8), :] = jnp.sin(angles)

    def dec_table(i, carry):
        row = pl.multiple_of(i * 8, 8)
        table(row, lens_v[pl.ds(row, 8), :])
        return carry

    def chunk_table(i, carry):
        row = pl.multiple_of(i * 8, 8)
        table(dec + row, lens_ref[dec] + row + lax.broadcasted_iota(jnp.int32, (8, LANES), 0))
        return carry

    lax.fori_loop(0, dec // 8, dec_table, 0)
    lax.fori_loop(0, chunk // 8, chunk_table, 0)

    def normalize(stream, src, gain):
        first, last = span[stream].start, span[stream].stop

        def block(i, carry):
            band = pl.ds(pl.multiple_of(first + i * 16, 16), 16)
            values = src[band, :].astype(F32)
            inv = lax.rsqrt(jnp.sum(values * values, axis=1, keepdims=True) * (1.0 / cols) + EPSILON)
            normed[band, :] = (values * inv * gain).astype(BF16)
            return carry

        lax.fori_loop(0, (last - first) // 16, block, 0, unroll=4)

    def rope(stream, values):
        wide = values.shape[1]
        lane = lax.broadcasted_iota(jnp.int32, values.shape, 1)
        turned = jnp.where(lane % head < head // 2, -pltpu.roll(values, wide - head // 2, 1), pltpu.roll(values, head // 2, 1))
        cos, sin = cos_t[span[stream], :], sin_t[span[stream], :]
        if wide > LANES:
            cos, sin = jnp.concatenate([cos, cos], axis=1), jnp.concatenate([sin, sin], axis=1)
        return (values * cos + turned * sin).astype(BF16).astype(F32)

    def project(stream, layer):
        values = normed[span[stream], :]
        q_t[span[stream], :] = rope(stream, matmul(values, wq[layer]).astype(BF16).astype(F32))
        kv = matmul_nt(values, wkv[layer]).astype(BF16)
        k_t[span[stream], :] = rope(stream, kv[:, :LANES].astype(F32))
        v_t[span[stream], :] = kv[:, LANES:].astype(F32)

    def decode_setup():
        lane = lax.broadcasted_iota(jnp.int32, (dec, LANES), 1)
        keys = k_t[0:dec, :]
        for pair in range(heads // 2):
            block = q_t[0:dec, pair * LANES:(pair + 1) * LANES]
            swapped = pltpu.roll(block, head, 1)
            product = block * keys
            for side in range(2):
                r = 2 * pair + side
                mine = (lane < head) if side == 0 else (lane >= head)
                self_t[r] = jnp.broadcast_to(jnp.sum(jnp.where(mine, product, 0.0), axis=1, keepdims=True) * scale, (dec, LANES))
                twice = jnp.where(mine, block, swapped)
                wide = jnp.concatenate([twice] * (SEQS * head // LANES), axis=1)
                col = lax.broadcasted_iota(jnp.int32, wide.shape, 1)
                row = lax.broadcasted_iota(jnp.int32, wide.shape, 0)
                qbd[r] = jnp.where(col // head == row % SEQS, wide, 0.0)

    def decode(bands):
        probs, own_probs = [], []
        for first in bands:
            band = slice(first, first + SEQS)
            queries = qbd[:, band, :].reshape(heads * SEQS, SEQS * head).astype(BF16)
            logits = matmul(queries, kbuf[band].reshape(SEQS * head, seq_len)) * scale
            logits = logits.reshape(heads, SEQS, seq_len)
            seen = lax.broadcasted_iota(jnp.int32, (SEQS, seq_len), 1) < lens_v[band, 0:1]
            logits = jnp.where(seen[None], logits, -jnp.inf)
            own = self_t[:, band, 0:1]
            top = jnp.maximum(jnp.max(logits, axis=2, keepdims=True), own)
            weights = jnp.exp(logits - top)
            own_weight = jnp.exp(own - top)
            inv = 1.0 / (jnp.sum(weights, axis=2, keepdims=True) + own_weight)
            probs.append((weights * inv).astype(BF16).reshape(heads * SEQS, seq_len))
            own_probs.append((own_weight * inv).astype(BF16).astype(F32))
        for first, prob, own_prob in zip(bands, probs, own_probs):
            band = slice(first, first + SEQS)
            mixed = matmul_nt(prob, vbuf[band].reshape(SEQS * head, seq_len))
            col = lax.broadcasted_iota(jnp.int32, mixed.shape, 1)
            row = lax.broadcasted_iota(jnp.int32, mixed.shape, 0)
            mixed = jnp.where(col // head == row % SEQS, mixed, 0.0)
            folded = mixed[:, 0:LANES]
            for i in range(1, SEQS * head // LANES):
                folded = folded + mixed[:, i * LANES:(i + 1) * LANES]
            folded = folded + pltpu.roll(folded, head, 1)
            result = folded.reshape(heads, SEQS, LANES) + own_prob * v_t[band, :][None]
            lane = lax.broadcasted_iota(jnp.int32, (SEQS, LANES), 1)
            att[band, 0:LANES] = jnp.where(lane < head, result[0], result[1])
            att[band, LANES:2 * LANES] = jnp.where(lane < head, result[2], result[3])

    def prefill_setup():
        lane = lax.broadcasted_iota(jnp.int32, (chunk, LANES), 1)
        for pair in range(heads // 2):
            block = q_t[dec:rows, pair * LANES:(pair + 1) * LANES]
            qh[2 * pair] = jnp.where(lane < head, block, 0.0).astype(BF16)
            qh[2 * pair + 1] = jnp.where(lane >= head, block, 0.0).astype(BF16)

    def prefill(r):
        queries = qh[r]
        keys = kbuf[dec]
        logits = matmul(queries, jnp.concatenate([keys, keys], axis=0)) * scale
        seen = lax.broadcasted_iota(jnp.int32, (chunk, seq_len), 1) < lens_ref[dec]
        logits = jnp.where(seen, logits, -jnp.inf)
        own = matmul_nt(queries, k_t[dec:rows, :].astype(BF16)) * scale
        causal = lax.broadcasted_iota(jnp.int32, (chunk, chunk), 1) <= lax.broadcasted_iota(jnp.int32, (chunk, chunk), 0)
        own = jnp.where(causal, own, -jnp.inf)
        top = jnp.maximum(jnp.max(logits, axis=1, keepdims=True), jnp.max(own, axis=1, keepdims=True))
        weights = jnp.exp(logits - top)
        own_weights = jnp.exp(own - top)
        inv = 1.0 / (jnp.sum(weights, axis=1, keepdims=True) + jnp.sum(own_weights, axis=1, keepdims=True))
        probs = (weights * inv).astype(BF16)
        own_probs = (own_weights * inv).astype(BF16)
        values = vbuf[dec]
        oh[r] = matmul_nt(probs, jnp.concatenate([values, values], axis=0)) + matmul(own_probs, v_t[dec:rows, :].astype(BF16))

    def prefill_end():
        lane = lax.broadcasted_iota(jnp.int32, (chunk, LANES), 1)
        for pair in range(heads // 2):
            att[dec:rows, pair * LANES:(pair + 1) * LANES] = jnp.where(lane < head, oh[2 * pair], oh[2 * pair + 1])

    def copy(src, dst, send, recv, to):
        return pltpu.make_async_remote_copy(src_ref=src, dst_ref=dst, send_sem=send, recv_sem=recv, device_id=to, device_id_type=MESH)

    def step_of(slot):
        high, low = slot // 2, slot % 2
        return 2 - low + high * (1 - 2 * low)

    greeted = []

    def sum_over_tp(stream, index, product, product_time, base, target):
        part = parts[stream]
        pair_in, pair_sum, ring_in = buffers[stream]
        band = span[stream]
        sems = index * 2 + stream
        scale_wire = (band.stop - band.start) / rows

        def piece_of(which_core, slot):
            return which_core * chips + at_chip(step_of(slot))

        def pair_copy(slot):
            return copy(part.at[piece_of(1 - core, slot)], pair_in.at[index, slot], pair_send.at[sems, slot], pair_recv.at[sems, slot], partner)

        def theirs(slot):
            piece = piece_of(1 - core, slot)
            part[piece] = product(piece).astype(BF16)

        def ours(slot):
            piece = piece_of(core, slot)
            part[piece] = product(piece).astype(BF16)

        if not greeted:
            greeted.append(True)
            pl.semaphore_wait(barrier, 4)
        for slot in range(4):
            theirs(slot)
        for slot in range(4):
            pair_copy(slot).start()
        for slot in range(4):
            ours(slot)
        yield product_time, 1.1 + 0.3 * scale_wire

        def columns(which_core, which_chip):
            return pl.ds(pl.multiple_of(which_core * half + which_chip * width, LANES), width)

        def pair_add(slot):
            return part[piece_of(core, slot)].astype(F32) + pair_in[index, slot].astype(F32)

        def scatter(slot):
            return copy(pair_sum.at[index, slot], ring_in.at[index, slot], ring_send.at[sems, slot], ring_recv.at[sems, slot], others[slot])

        def gather(slot):
            block = target.at[band, columns(core, chip)]
            return copy(block, block, gather_send.at[sems, slot], gather_recv.at[sems, slot], others[slot])

        def share(step, slot):
            block = target.at[band, columns(core, at_chip(step))]
            return copy(block, block, share_send.at[sems, slot], share_recv.at[sems, slot], partner)

        for slot in range(3):
            pair_copy(slot).wait_recv()
            pair_sum[index, slot] = pair_add(slot).astype(BF16)
            scatter(slot).start()
        yield 0.25, FAR_WAIT + FAR_WIRE * scale_wire
        pair_copy(3).wait_recv()
        total = pair_add(3) + base[band, columns(core, chip)].astype(F32)
        for slot in (1, 2, 0):
            scatter(slot).wait_recv()
            total = total + ring_in[index, slot].astype(F32)
        target[band, columns(core, chip)] = total.astype(BF16)
        for slot in range(3):
            gather(slot).start()
        share(0, 3).start()
        yield 0.25, NEAR_WAIT + NEAR_WIRE * scale_wire
        for slot, step in ((1, -1), (2, 1)):
            gather(slot).wait_recv()
            share(step, slot).start()
        yield 0.05, FAR_WAIT - NEAR_WAIT + (FAR_WIRE - NEAR_WIRE) * scale_wire
        gather(0).wait_recv()
        share(2, 0).start()
        yield 0.05, 1.0 + 0.2 * scale_wire
        for slot in range(4):
            share(0, slot).wait_recv()
        for slot in range(4):
            pair_copy(slot).wait_send()
            share(0, slot).wait_send()
        for slot in range(3):
            scatter(slot).wait_send()
            gather(slot).wait_send()

    def piece_columns(piece):
        return pl.ds(pl.multiple_of(piece * width, LANES), width)

    attended = [0] * layers

    def attention_done(layer):
        attended[layer] += 1
        if attended[layer] == 2 and layer + 1 < layers:
            start(layer + 1, projections)
            start_cache(layer + 1, [loads])
            start(layer + 1, ('o',))
            start_cache(layer + 1, range(loads))
            start(layer + 1, ('g', 'u', 'd'))

    def stream_steps(stream):
        band = span[stream]
        residual = x_ref
        for layer in range(layers):
            normalize(stream, residual, again_ref[...].astype(F32)[layer:layer + 1])
            yield 0.3, 0.0
            arrive(layer, projections)
            if layer == 0 and stream == 1:
                start_cache(0, range(loads))
            project(stream, layer)
            if stream == 0:
                decode_setup()
                yield 1.0, 0.0
                for index in range(loads):
                    arrive_cache(layer, index)
                    decode(range(index * load_seqs, (index + 1) * load_seqs, SEQS))
                    yield 1.4, 0.0
            else:
                prefill_setup()
                yield 0.8, 0.0
                arrive_cache(layer, loads)
                for r in range(heads):
                    prefill(r)
                    yield 0.55, 0.0
                prefill_end()
                if layer == 0:
                    start(layer, ('g', 'u', 'd'))
            attention_done(layer)
            arrive(layer, ('o',))
            target = hid.at[2 * layer]
            yield from sum_over_tp(stream, 2 * layer, lambda piece: matmul(att[band, :].astype(BF16), wo[layer, :, piece_columns(piece)]), 0.3, residual, target)
            residual = target
            normalize(stream, residual, mgain_ref[...].astype(F32)[layer:layer + 1])
            arrive(layer, ('g', 'u'))

            def mlp_step(i, carry):
                piece = piece_columns(i)
                gate = matmul(normed[band, :], wg[layer, :, piece])
                up = matmul(normed[band, :], wu[layer, :, piece])
                act[band, piece] = (gate / (1.0 + jnp.exp(-gate)) * up).astype(BF16)
                return carry

            lax.fori_loop(0, act.shape[1] // width, mlp_step, 0, unroll=2)
            yield 1.4, 0.0
            arrive(layer, ('d',))
            target = out_ref if layer + 1 == layers else hid.at[2 * layer + 1]
            yield from sum_over_tp(stream, 2 * layer + 1, lambda piece: matmul(act[band, :], wd[layer, :, piece_columns(piece)]), 0.6, residual, target)
            residual = target

    run_streams([stream_steps(1), stream_steps(0)])


def run_layers(x, lengths, attn_gain, w_q, w_k, w_v, w_o, mlp_gain, w_gate, w_up, w_down, k_cache, v_cache, tp_size):
    rows, cols = x.shape
    layers = w_q.shape[0]
    head = k_cache.shape[-1]
    seqs, seq_len = k_cache.shape[1], k_cache.shape[3]
    dec = seqs - 1
    chunk = rows - dec
    heads = w_q.shape[2] // head
    inner = w_gate.shape[2]
    width = cols // tp_size
    sums = 2 * layers
    freq = jnp.power(ROPE_BASE, -jnp.arange(0, head, 2, dtype=F32) / head)
    freq = jnp.broadcast_to(jnp.tile(freq, LANES // (head // 2))[None], (8, LANES))
    turned = lambda array: jnp.swapaxes(array, -1, -2)
    k_cols, v_cols = turned(k_cache)[:, :, 0], turned(v_cache)[:, :, 0]
    dma = pltpu.SemaphoreType.DMA
    vmem = pl.BlockSpec(memory_space=pltpu.VMEM)
    hbm = pl.BlockSpec(memory_space=pl.ANY)
    scratch = [
        ((layers, cols, heads * head), BF16), ((layers, 4 * head, cols), BF16), ((layers, heads * head, cols), BF16),
        ((layers, cols, inner), BF16), ((layers, cols, inner), BF16), ((layers, inner, cols), BF16),
        ((seqs, head, seq_len), BF16), ((seqs, head, seq_len), BF16),
        ((sums - 1, rows, cols), BF16), ((rows, cols), BF16), ((rows, inner), BF16),
        ((dec, LANES), jnp.int32), ((rows, LANES), F32), ((rows, LANES), F32),
        ((rows, heads * head), F32), ((rows, LANES), F32), ((rows, LANES), F32),
        ((heads, dec, LANES), F32), ((heads, dec, SEQS * head), F32), ((heads, chunk, LANES), BF16), ((heads, chunk, LANES), F32),
        ((rows, heads * head), F32),
    ]
    for band in (dec, chunk):
        scratch += [((tp_size, band, width), BF16), ((sums, 4, band, width), BF16), ((sums, 3, band, width), BF16), ((sums, 3, band, width), BF16)]
    semaphores = [(layers, 9), (layers, 2, CACHE_LOADS + 1)] + [(2 * sums, count) for count in (4, 4, 3, 3, 3, 3, 4, 4)]
    return pl.pallas_call(
        functools.partial(layer_kernel, tp_size // 2),
        out_shape=jax.ShapeDtypeStruct(x.shape, x.dtype),
        in_specs=[vmem, pl.BlockSpec(memory_space=pltpu.SMEM), vmem, vmem, vmem] + [hbm] * 9,
        out_specs=vmem,
        scratch_shapes=[pltpu.VMEM(shape, dtype) for shape, dtype in scratch] + [dma(shape) for shape in semaphores],
        compiler_params=pltpu.CompilerParams(collective_id=0, has_side_effects=True, vmem_limit_bytes=VMEM_LIMIT),
    )(x, lengths, freq, attn_gain, mlp_gain, w_q, turned(w_k), turned(w_v), w_o, w_gate, w_up, w_down, k_cols, v_cols)


def solution(mesh):
    col_spec = P(None, None, 'tp')
    row_spec = P(None, 'tp', None)
    cache_spec = P(None, 'dp', 'tp', None, None)
    in_specs = (P('dp', None), P('dp'), P(), col_spec, col_spec, col_spec, row_spec, P(), col_spec, col_spec, row_spec, cache_spec, cache_spec)
    body = functools.partial(run_layers, tp_size=mesh.shape['tp'])
    return jax.shard_map(body, mesh=mesh, in_specs=in_specs, out_specs=P('dp', None), check_vma=False)
```

```python
import functools
import math

import jax
import jax.numpy as jnp
from jax import lax
from jax.experimental import pallas as pl
from jax.experimental.pallas import tpu as pltpu
from jax.sharding import PartitionSpec as P

ROPE_BASE = 500000.0
EPSILON = 1e-5
MESH = pl.DeviceIdType.MESH
LANES = 128
SEQS = 8
CACHE_LOADS = 4
NEAR_WAIT, NEAR_WIRE, FAR_WAIT, FAR_WIRE = 2.4, 1.4, 3.0, 2.8
VMEM_LIMIT = 67043328
F32 = jnp.float32
BF16 = jnp.bfloat16
NT = (((1,), (1,)), ((), ()))


def matmul(a, b):
    return jnp.dot(a, b, preferred_element_type=F32)


def matmul_nt(a, b):
    return lax.dot_general(a, b, NT, preferred_element_type=F32)


def run_streams(streams):
    now, ready = 0.0, [0.0] * len(streams)
    arrived = [False] * len(streams)
    live = set(range(len(streams)))

    def order(i):
        return (0, 0, ready[i]) if ready[i] <= now and arrived[i] else (0, 1, i) if ready[i] <= now else (1, ready[i], i)

    while live:
        pick = min(sorted(live), key=order)
        now = max(now, ready[pick])
        try:
            busy, wait = next(streams[pick])
        except StopIteration:
            live.discard(pick)
            continue
        now += busy
        ready[pick] = now + wait
        arrived[pick] = wait > 0


def layer_kernel(chips, x_hbm, lens_ref, again_ref, mgain_ref, wq_hbm, wk_hbm, wv_hbm, wo_hbm, wg_hbm, wu_hbm, wd_hbm, k_hbm, v_hbm,
                 out_ref,
                 x_ref, wq, wkv, wo, wg, wu, wd, kbuf, vbuf, hid, normed, act, lens_v, cos_t, sin_t, q_t, k_t, v_t, self_t, qbd, qh, oh, att,
                 part_a, pair_in_a, pair_sum_a, ring_in_a, part_b, pair_in_b, pair_sum_b, ring_in_b,
                 io_sem, load_sem, cache_sem, pair_send, pair_recv, ring_send, ring_recv, gather_send, gather_recv, share_send, share_recv):
    layers = wq.shape[0]
    rows, cols = x_hbm.shape
    dec = lens_v.shape[0]
    chunk = rows - dec
    head = k_hbm.shape[2]
    seq_len = k_hbm.shape[3]
    heads = qbd.shape[0]
    scale = head ** -0.5
    loads = cache_sem.shape[2] - 1
    load_seqs = dec // loads
    half = cols // 2
    width = half // chips
    span = (slice(0, dec), slice(dec, rows))
    parts = (part_a, part_b)
    buffers = ((pair_in_a, pair_sum_a, ring_in_a), (pair_in_b, pair_sum_b, ring_in_b))

    me = lax.axis_index('tp')
    core, chip = lax.rem(me, 2), lax.div(me, 2)

    def at_chip(step):
        return lax.rem(chip + step + chips, chips)

    partner = {'tp': chip * 2 + 1 - core}
    right = {'tp': at_chip(1) * 2 + core}
    left = {'tp': at_chip(-1) * 2 + core}
    far = {'tp': at_chip(2) * 2 + core}
    others = (far, right, left)

    def load(layer, name):
        src, dst, slot = {
            'q': (wq_hbm.at[layer], wq.at[layer], 0),
            'k0': (wk_hbm.at[layer], wkv.at[layer, 0:head], 1),
            'k1': (wk_hbm.at[layer], wkv.at[layer, head:2 * head], 2),
            'v0': (wv_hbm.at[layer], wkv.at[layer, 2 * head:3 * head], 3),
            'v1': (wv_hbm.at[layer], wkv.at[layer, 3 * head:4 * head], 4),
            'o': (wo_hbm.at[layer], wo.at[layer], 5),
            'g': (wg_hbm.at[layer], wg.at[layer], 6),
            'u': (wu_hbm.at[layer], wu.at[layer], 7),
            'd': (wd_hbm.at[layer], wd.at[layer], 8),
        }[name]
        return pltpu.make_async_copy(src, dst, load_sem.at[layer, slot])

    def cache_load(layer, which, index):
        src, dst = ((k_hbm, kbuf), (v_hbm, vbuf))[which]
        block = pl.ds(index * load_seqs, load_seqs) if index < loads else dec
        return pltpu.make_async_copy(src.at[layer, block], dst.at[block], cache_sem.at[layer, which, index])

    landed = set()

    def arrive(layer, names):
        for name in names:
            if (layer, name) not in landed:
                landed.add((layer, name))
                load(layer, name).wait()

    def arrive_cache(layer, index):
        for which in range(2):
            cache_load(layer, which, index).wait()

    def start(layer, names):
        for name in names:
            load(layer, name).start()

    def start_cache(layer, indices):
        for index in indices:
            for which in range(2):
                cache_load(layer, which, index).start()

    projections = ('q', 'k0', 'k1', 'v0', 'v1')
    x_loads = [pltpu.make_async_copy(x_hbm.at[band], x_ref.at[band], io_sem.at[side]) for side, band in enumerate(span)]
    x_loads[1].start()
    start(0, projections)
    x_loads[0].start()
    start_cache(0, [loads])
    start(0, ('o',))

    barrier = pltpu.get_barrier_semaphore()
    for device in (partner, right, left, far):
        pl.semaphore_signal(barrier, inc=1, device_id=device, device_id_type=MESH)

    def fill(row, carry):
        lens_v[pl.ds(row, 1), :] = jnp.full((1, LANES), lens_ref[row], jnp.int32)
        return carry

    lax.fori_loop(0, dec, fill, 0)

    pair_ids = (lax.broadcasted_iota(jnp.int32, (8, LANES), 1) % (head // 2)).astype(F32)
    freq = jnp.exp(pair_ids * (-2.0 * math.log(ROPE_BASE) / head))

    def table(row, positions):
        angles = positions.astype(F32) * freq
        cos_t[pl.ds(row, 8), :] = jnp.cos(angles)
        sin_t[pl.ds(row, 8), :] = jnp.sin(angles)

    def dec_table(i, carry):
        row = pl.multiple_of(i * 8, 8)
        table(row, lens_v[pl.ds(row, 8), :])
        return carry

    def chunk_table(i, carry):
        row = pl.multiple_of(i * 8, 8)
        table(dec + row, lens_ref[dec] + row + lax.broadcasted_iota(jnp.int32, (8, LANES), 0))
        return carry

    lax.fori_loop(0, dec // 8, dec_table, 0)
    lax.fori_loop(0, chunk // 8, chunk_table, 0)

    def normalize(stream, src, gain):
        first, last = span[stream].start, span[stream].stop

        def block(i, carry):
            band = pl.ds(pl.multiple_of(first + i * 16, 16), 16)
            values = src[band, :].astype(F32)
            inv = lax.rsqrt(jnp.sum(values * values, axis=1, keepdims=True) * (1.0 / cols) + EPSILON)
            normed[band, :] = (values * inv * gain).astype(BF16)
            return carry

        lax.fori_loop(0, (last - first) // 16, block, 0, unroll=4)

    def rope(stream, values):
        wide = values.shape[1]
        lane = lax.broadcasted_iota(jnp.int32, values.shape, 1)
        turned = jnp.where(lane % head < head // 2, -pltpu.roll(values, wide - head // 2, 1), pltpu.roll(values, head // 2, 1))
        cos, sin = cos_t[span[stream], :], sin_t[span[stream], :]
        if wide > LANES:
            cos, sin = jnp.concatenate([cos, cos], axis=1), jnp.concatenate([sin, sin], axis=1)
        return (values * cos + turned * sin).astype(BF16).astype(F32)

    def project(stream, layer):
        values = normed[span[stream], :]
        q_t[span[stream], :] = rope(stream, matmul(values, wq[layer]).astype(BF16).astype(F32))
        kv = matmul_nt(values, wkv[layer]).astype(BF16)
        k_t[span[stream], :] = rope(stream, kv[:, :LANES].astype(F32))
        v_t[span[stream], :] = kv[:, LANES:].astype(F32)

    def decode_setup():
        lane = lax.broadcasted_iota(jnp.int32, (dec, LANES), 1)
        keys = k_t[0:dec, :]
        for pair in range(heads // 2):
            block = q_t[0:dec, pair * LANES:(pair + 1) * LANES]
            swapped = pltpu.roll(block, head, 1)
            product = block * keys
            for side in range(2):
                r = 2 * pair + side
                mine = (lane < head) if side == 0 else (lane >= head)
                self_t[r] = jnp.broadcast_to(jnp.sum(jnp.where(mine, product, 0.0), axis=1, keepdims=True) * scale, (dec, LANES))
                twice = jnp.where(mine, block, swapped)
                wide = jnp.concatenate([twice] * (SEQS * head // LANES), axis=1)
                col = lax.broadcasted_iota(jnp.int32, wide.shape, 1)
                row = lax.broadcasted_iota(jnp.int32, wide.shape, 0)
                qbd[r] = jnp.where(col // head == row % SEQS, wide, 0.0)

    def decode(bands):
        probs, own_probs = [], []
        for first in bands:
            band = slice(first, first + SEQS)
            queries = qbd[:, band, :].reshape(heads * SEQS, SEQS * head).astype(BF16)
            logits = matmul(queries, kbuf[band].reshape(SEQS * head, seq_len)) * scale
            logits = logits.reshape(heads, SEQS, seq_len)
            seen = lax.broadcasted_iota(jnp.int32, (SEQS, seq_len), 1) < lens_v[band, 0:1]
            logits = jnp.where(seen[None], logits, -jnp.inf)
            own = self_t[:, band, 0:1]
            top = jnp.maximum(jnp.max(logits, axis=2, keepdims=True), own)
            weights = jnp.exp(logits - top)
            own_weight = jnp.exp(own - top)
            inv = 1.0 / (jnp.sum(weights, axis=2, keepdims=True) + own_weight)
            probs.append((weights * inv).astype(BF16).reshape(heads * SEQS, seq_len))
            own_probs.append((own_weight * inv).astype(BF16).astype(F32))
        for first, prob, own_prob in zip(bands, probs, own_probs):
            band = slice(first, first + SEQS)
            mixed = matmul_nt(prob, vbuf[band].reshape(SEQS * head, seq_len))
            col = lax.broadcasted_iota(jnp.int32, mixed.shape, 1)
            row = lax.broadcasted_iota(jnp.int32, mixed.shape, 0)
            mixed = jnp.where(col // head == row % SEQS, mixed, 0.0)
            folded = mixed[:, 0:LANES]
            for i in range(1, SEQS * head // LANES):
                folded = folded + mixed[:, i * LANES:(i + 1) * LANES]
            folded = folded + pltpu.roll(folded, head, 1)
            result = folded.reshape(heads, SEQS, LANES) + own_prob * v_t[band, :][None]
            lane = lax.broadcasted_iota(jnp.int32, (SEQS, LANES), 1)
            att[band, 0:LANES] = jnp.where(lane < head, result[0], result[1])
            att[band, LANES:2 * LANES] = jnp.where(lane < head, result[2], result[3])

    def prefill_setup():
        lane = lax.broadcasted_iota(jnp.int32, (chunk, LANES), 1)
        for pair in range(heads // 2):
            block = q_t[dec:rows, pair * LANES:(pair + 1) * LANES]
            qh[2 * pair] = jnp.where(lane < head, block, 0.0).astype(BF16)
            qh[2 * pair + 1] = jnp.where(lane >= head, block, 0.0).astype(BF16)

    def prefill(r):
        queries = qh[r]
        keys = kbuf[dec]
        logits = matmul(queries, jnp.concatenate([keys, keys], axis=0)) * scale
        seen = lax.broadcasted_iota(jnp.int32, (chunk, seq_len), 1) < lens_ref[dec]
        logits = jnp.where(seen, logits, -jnp.inf)
        own = matmul_nt(queries, k_t[dec:rows, :].astype(BF16)) * scale
        causal = lax.broadcasted_iota(jnp.int32, (chunk, chunk), 1) <= lax.broadcasted_iota(jnp.int32, (chunk, chunk), 0)
        own = jnp.where(causal, own, -jnp.inf)
        top = jnp.maximum(jnp.max(logits, axis=1, keepdims=True), jnp.max(own, axis=1, keepdims=True))
        weights = jnp.exp(logits - top)
        own_weights = jnp.exp(own - top)
        inv = 1.0 / (jnp.sum(weights, axis=1, keepdims=True) + jnp.sum(own_weights, axis=1, keepdims=True))
        probs = (weights * inv).astype(BF16)
        own_probs = (own_weights * inv).astype(BF16)
        values = vbuf[dec]
        oh[r] = matmul_nt(probs, jnp.concatenate([values, values], axis=0)) + matmul(own_probs, v_t[dec:rows, :].astype(BF16))

    def prefill_end():
        lane = lax.broadcasted_iota(jnp.int32, (chunk, LANES), 1)
        for pair in range(heads // 2):
            att[dec:rows, pair * LANES:(pair + 1) * LANES] = jnp.where(lane < head, oh[2 * pair], oh[2 * pair + 1])

    def copy(src, dst, send, recv, to):
        return pltpu.make_async_remote_copy(src_ref=src, dst_ref=dst, send_sem=send, recv_sem=recv, device_id=to, device_id_type=MESH)

    def step_of(slot):
        high, low = slot // 2, slot % 2
        return 2 - low + high * (1 - 2 * low)

    greeted = []

    def sum_over_tp(stream, index, product, product_time, base, target):
        part = parts[stream]
        pair_in, pair_sum, ring_in = buffers[stream]
        band = span[stream]
        sems = index * 2 + stream
        scale_wire = (band.stop - band.start) / rows

        def piece_of(which_core, slot):
            return which_core * chips + at_chip(step_of(slot))

        def pair_copy(slot):
            return copy(part.at[piece_of(1 - core, slot)], pair_in.at[index, slot], pair_send.at[sems, slot], pair_recv.at[sems, slot], partner)

        def theirs(slot):
            piece = piece_of(1 - core, slot)
            part[piece] = product(piece).astype(BF16)

        def ours(slot):
            piece = piece_of(core, slot)
            part[piece] = product(piece).astype(BF16)

        if not greeted:
            greeted.append(True)
            pl.semaphore_wait(barrier, 4)
        for slot in range(4):
            theirs(slot)
        for slot in range(4):
            pair_copy(slot).start()
        for slot in range(4):
            ours(slot)
        yield product_time, 1.1 + 0.3 * scale_wire

        def columns(which_core, which_chip):
            return pl.ds(pl.multiple_of(which_core * half + which_chip * width, LANES), width)

        def pair_add(slot):
            return part[piece_of(core, slot)].astype(F32) + pair_in[index, slot].astype(F32)

        def scatter(slot):
            return copy(pair_sum.at[index, slot], ring_in.at[index, slot], ring_send.at[sems, slot], ring_recv.at[sems, slot], others[slot])

        def gather(slot):
            block = target.at[band, columns(core, chip)]
            return copy(block, block, gather_send.at[sems, slot], gather_recv.at[sems, slot], others[slot])

        def share(step, slot):
            block = target.at[band, columns(core, at_chip(step))]
            return copy(block, block, share_send.at[sems, slot], share_recv.at[sems, slot], partner)

        for slot in range(3):
            pair_copy(slot).wait_recv()
            pair_sum[index, slot] = pair_add(slot).astype(BF16)
            scatter(slot).start()
        yield 0.25, FAR_WAIT + FAR_WIRE * scale_wire
        pair_copy(3).wait_recv()
        total = pair_add(3) + base[band, columns(core, chip)].astype(F32)
        for slot in (1, 2, 0):
            scatter(slot).wait_recv()
            total = total + ring_in[index, slot].astype(F32)
        target[band, columns(core, chip)] = total.astype(BF16)
        for slot in range(3):
            gather(slot).start()
        share(0, 3).start()
        yield 0.25, NEAR_WAIT + NEAR_WIRE * scale_wire
        for slot, step in ((1, -1), (2, 1)):
            gather(slot).wait_recv()
            share(step, slot).start()
        yield 0.05, FAR_WAIT - NEAR_WAIT + (FAR_WIRE - NEAR_WIRE) * scale_wire
        gather(0).wait_recv()
        share(2, 0).start()
        yield 0.05, 1.0 + 0.2 * scale_wire
        for slot in range(4):
            share(0, slot).wait_recv()
        for slot in range(4):
            pair_copy(slot).wait_send()
            share(0, slot).wait_send()
        for slot in range(3):
            scatter(slot).wait_send()
            gather(slot).wait_send()

    def piece_columns(piece):
        return pl.ds(pl.multiple_of(piece * width, LANES), width)

    attended = [0] * layers

    def attention_done(layer):
        attended[layer] += 1
        if attended[layer] == 2 and layer + 1 < layers:
            start(layer + 1, projections)
            start_cache(layer + 1, [loads])
            start(layer + 1, ('o',))
            start_cache(layer + 1, range(loads))
            start(layer + 1, ('g', 'u', 'd'))

    def stream_steps(stream):
        band = span[stream]
        residual = x_ref
        x_loads[stream].wait()
        for layer in range(layers):
            normalize(stream, residual, again_ref[...].astype(F32)[layer:layer + 1])
            yield 0.3, 0.0
            arrive(layer, projections)
            if layer == 0 and stream == 1:
                start_cache(0, range(loads))
            project(stream, layer)
            if stream == 0:
                decode_setup()
                yield 1.0, 0.0
                for index in range(loads):
                    arrive_cache(layer, index)
                    decode(range(index * load_seqs, (index + 1) * load_seqs, SEQS))
                    yield 1.4, 0.0
            else:
                prefill_setup()
                yield 0.8, 0.0
                arrive_cache(layer, loads)
                for r in range(heads):
                    prefill(r)
                    yield 0.55, 0.0
                prefill_end()
                if layer == 0:
                    start(layer, ('g', 'u', 'd'))
            attention_done(layer)
            arrive(layer, ('o',))
            target = hid.at[2 * layer]
            yield from sum_over_tp(stream, 2 * layer, lambda piece: matmul(att[band, :].astype(BF16), wo[layer, :, piece_columns(piece)]), 0.3, residual, target)
            residual = target
            normalize(stream, residual, mgain_ref[...].astype(F32)[layer:layer + 1])
            arrive(layer, ('g', 'u'))

            def mlp_step(i, carry):
                piece = piece_columns(i)
                gate = matmul(normed[band, :], wg[layer, :, piece])
                up = matmul(normed[band, :], wu[layer, :, piece])
                act[band, piece] = (gate / (1.0 + jnp.exp(-gate)) * up).astype(BF16)
                return carry

            lax.fori_loop(0, act.shape[1] // width, mlp_step, 0, unroll=4)
            yield 1.4, 0.0
            arrive(layer, ('d',))
            target = hid.at[2 * layer + 1]
            yield from sum_over_tp(stream, 2 * layer + 1, lambda piece: matmul(act[band, :], wd[layer, :, piece_columns(piece)]), 0.6, residual, target)
            residual = target
        stores.append(pltpu.make_async_copy(residual.at[band], out_ref.at[band], io_sem.at[2 + stream]))
        stores[-1].start()

    stores = []
    run_streams([stream_steps(1), stream_steps(0)])
    for each in stores:
        each.wait()


def run_layers(x, lengths, attn_gain, w_q, w_k, w_v, w_o, mlp_gain, w_gate, w_up, w_down, k_cache, v_cache, tp_size):
    rows, cols = x.shape
    layers = w_q.shape[0]
    head = k_cache.shape[-1]
    seqs, seq_len = k_cache.shape[1], k_cache.shape[3]
    dec = seqs - 1
    chunk = rows - dec
    heads = w_q.shape[2] // head
    inner = w_gate.shape[2]
    width = cols // tp_size
    sums = 2 * layers
    turned = lambda array: jnp.swapaxes(array, -1, -2)
    k_cols, v_cols = turned(k_cache)[:, :, 0], turned(v_cache)[:, :, 0]
    dma = pltpu.SemaphoreType.DMA
    vmem = pl.BlockSpec(memory_space=pltpu.VMEM)
    hbm = pl.BlockSpec(memory_space=pl.ANY)
    scratch = [
        ((rows, cols), BF16),
        ((layers, cols, heads * head), BF16), ((layers, 4 * head, cols), BF16), ((layers, heads * head, cols), BF16),
        ((layers, cols, inner), BF16), ((layers, cols, inner), BF16), ((layers, inner, cols), BF16),
        ((seqs, head, seq_len), BF16), ((seqs, head, seq_len), BF16),
        ((sums, rows, cols), BF16), ((rows, cols), BF16), ((rows, inner), BF16),
        ((dec, LANES), jnp.int32), ((rows, LANES), F32), ((rows, LANES), F32),
        ((rows, heads * head), F32), ((rows, LANES), F32), ((rows, LANES), F32),
        ((heads, dec, LANES), F32), ((heads, dec, SEQS * head), F32), ((heads, chunk, LANES), BF16), ((heads, chunk, LANES), F32),
        ((rows, heads * head), F32),
    ]
    for band in (dec, chunk):
        scratch += [((tp_size, band, width), BF16), ((sums, 4, band, width), BF16), ((sums, 3, band, width), BF16), ((sums, 3, band, width), BF16)]
    semaphores = [(4,), (layers, 9), (layers, 2, CACHE_LOADS + 1)] + [(2 * sums, count) for count in (4, 4, 3, 3, 3, 3, 4, 4)]
    return pl.pallas_call(
        functools.partial(layer_kernel, tp_size // 2),
        out_shape=jax.ShapeDtypeStruct(x.shape, x.dtype),
        in_specs=[hbm, pl.BlockSpec(memory_space=pltpu.SMEM), vmem, vmem] + [hbm] * 9,
        out_specs=hbm,
        scratch_shapes=[pltpu.VMEM(shape, dtype) for shape, dtype in scratch] + [dma(shape) for shape in semaphores],
        compiler_params=pltpu.CompilerParams(collective_id=0, has_side_effects=True, vmem_limit_bytes=VMEM_LIMIT),
    )(x, lengths, attn_gain, mlp_gain, w_q, turned(w_k), turned(w_v), w_o, w_gate, w_up, w_down, k_cols, v_cols)


def solution(mesh):
    col_spec = P(None, None, 'tp')
    row_spec = P(None, 'tp', None)
    cache_spec = P(None, 'dp', 'tp', None, None)
    in_specs = (P('dp', None), P('dp'), P(), col_spec, col_spec, col_spec, row_spec, P(), col_spec, col_spec, row_spec, cache_spec, cache_spec)
    body = functools.partial(run_layers, tp_size=mesh.shape['tp'])
    return jax.shard_map(body, mesh=mesh, in_specs=in_specs, out_specs=P('dp', None), check_vma=False)
```
